32 devices in a mesh: section: 2 (over core), dp: 4 (over y, x), tensor: 4 (over z).
Axes of the slice: x: 2, y: 2, z: 4, core: 2. Of those that a mesh axis runs over, the one named last changes fastest.
Arguments:
- tokens_in: bfloat16 [512, 8192], P('dp', ('section', 'tensor')), may hold values from -70 to 70
- gain_attn: bfloat16 [8192], replicated, may hold values from 0.5 to 1.5
- w_query: bfloat16 [8192, 8192], P(None, ('section', 'tensor')), may hold values from -6 to 6
- w_keyval: bfloat16 [8192, 2048], P(None, ('section', 'tensor')), may hold values from -0.0625 to 0.0625
- w_out: bfloat16 [8192, 8192], P(('section', 'tensor')), may hold values from -0.0625 to 0.0625
- gain_mlp: bfloat16 [8192], replicated, may hold values from 0.5 to 1.5
- w_gate: bfloat16 [8192, 16384], P('dp', ('section', 'tensor')), may hold values from -0.0625 to 0.0625
- w_up: bfloat16 [8192, 16384], P('dp', ('section', 'tensor')), may hold values from -0.0625 to 0.0625
- w_down: bfloat16 [16384, 8192], P(('section', 'tensor'), 'dp'), may hold values from -0.046875 to 0.046875
Outputs:
- layer_out: bfloat16 [512, 8192], P(('section', 'tensor'), 'dp')
The draws below stay inside these ranges and needn't reach their ends.
All inputs are finite; a program needn't handle non-finite values.
Results may differ from the reference program's by a relative error of at most 0.0068.
Values may be sent and summed in bfloat16 or wider, within the bound.
A program may use at most 128 MiB of HBM per device.

```python
import math
import jax
import jax.numpy as jnp
from jax import lax

D = 8192
H = 64
KVH = 8
HD = 128
FF = 16384
TOKENS = 512


def draw_tokens_in(key, part):
    first_key, scale_key = jax.random.split(jax.random.fold_in(key, 11), 2)
    base_values = jnp.clip(jax.random.normal(first_key, (TOKENS, D), jnp.float32), -6.0, 6.0)
    scales = jnp.exp(jax.random.uniform(scale_key, (TOKENS, 1), jnp.float32, math.log(0.3), math.log(3.0)))
    values = scales * base_values
    return values.astype(jnp.bfloat16)


def draw_w_query(key, part):
    entry_key, head_key = jax.random.split(jax.random.fold_in(key, 23), 2)
    base_values = jnp.clip(jax.random.normal(entry_key, (D, H * HD), jnp.float32), -6.0, 6.0) * D ** (-0.5)
    head_scale = jnp.exp(jax.random.uniform(head_key, (H,), jnp.float32, 0.0, math.log(3.0)))
    values = base_values * jnp.repeat(head_scale, HD)[None, :]
    values = jnp.clip(values, -6.0, 6.0)
    return values.astype(jnp.bfloat16)


def block_levels(own_key, extent, pieces, smallest, high):
    factor_of = 1.0
    for dim, parts in pieces:
        steps = jax.random.uniform(jax.random.fold_in(jax.random.fold_in(own_key, 6), dim), (parts,), jnp.float32, smallest / len(pieces), high / len(pieces))
        factor_of = factor_of * jnp.repeat(jnp.exp(steps), extent[dim] // parts).reshape((-1,) + (1,) * (len(extent) - 1 - dim))
    return factor_of


def noise(stream_key, dims, width, limit, shards=(), kind=jnp.bfloat16):
    entries = width * jax.random.normal(stream_key, dims, jnp.float32)
    if shards:
        entries = entries * block_levels(stream_key, dims, shards, -0.22, 0.18)
    return jnp.clip(entries, -limit, limit).astype(kind)


def setup_inputs(seed: int = 0) -> dict:
    arg_keys = jax.random.split(jax.random.key(seed), 10)
    tokens_in = draw_tokens_in(jax.random.fold_in(arg_keys[9], 71), 0)
    gain_attn = jnp.clip(1.0 + 0.1 * jax.random.normal(arg_keys[1], (D,), jnp.float32), 0.5, 1.5).astype(jnp.bfloat16)
    w_query = draw_w_query(jax.random.fold_in(arg_keys[9], 71), 0)
    w_keyval = noise(arg_keys[3], (D, 2 * KVH * HD), D ** -0.5, 0.0625, ((1, 8),))
    w_out = noise(arg_keys[4], (H * HD, D), (H * HD) ** -0.5, 0.0625, ((0, 8),))
    gain_mlp = jnp.clip(1.0 + 0.1 * jax.random.normal(arg_keys[5], (D,), jnp.float32), 0.5, 1.5).astype(jnp.bfloat16)
    w_gate = noise(arg_keys[6], (D, FF), D ** -0.5, 0.0625, ((0, 4), (1, 8)))
    w_up = noise(arg_keys[7], (D, FF), D ** -0.5, 0.0625, ((0, 4), (1, 8)))
    w_down = noise(arg_keys[8], (FF, D), FF ** -0.5, 0.046875, ((0, 8), (1, 4)))
    return {"tokens_in": tokens_in, "gain_attn": gain_attn, "w_query": w_query, "w_keyval": w_keyval, "w_out": w_out, "gain_mlp": gain_mlp, "w_gate": w_gate, "w_up": w_up, "w_down": w_down}


EPS = 1e-05
THETA = 10000.0

def rms_scale(row_data, gain_row):
    values = row_data.astype(jnp.float32)
    factor = lax.rsqrt(lax.optimization_barrier(jnp.mean(values * values, axis=-1, keepdims=True)) + EPS)
    return (values * factor * gain_row.astype(jnp.float32)).astype(jnp.bfloat16)

def rotary(values, positions):
    half_dim = values.shape[-1] // 2
    frequency = THETA ** (-jnp.arange(half_dim, dtype=jnp.float32) * 2.0 / values.shape[-1])
    angles = positions.astype(jnp.float32)[:, None] * frequency[None, :]
    cosine = jnp.cos(angles)[:, None, :]
    sine_part = jnp.sin(angles)[:, None, :]
    first_half = values[..., :half_dim]
    second = values[..., half_dim:]
    return jnp.concatenate([first_half * cosine - second * sine_part, second * cosine + first_half * sine_part], axis=-1)

def reference(tokens_in, gain_attn, w_query, w_keyval, w_out, gain_mlp, w_gate, w_up, w_down):
    total_rows = tokens_in.shape[0]
    normed_attn = rms_scale(tokens_in, gain_attn)
    positions = jnp.arange(total_rows, dtype=jnp.int32)
    query_proj = jnp.dot(normed_attn, w_query, preferred_element_type=jnp.float32)
    query_rot = rotary(query_proj.reshape(total_rows, H, HD), positions).astype(jnp.bfloat16)
    keyval = jnp.dot(normed_attn, w_keyval, preferred_element_type=jnp.float32).astype(jnp.bfloat16)
    key_rot = rotary(keyval[:, :KVH * HD].astype(jnp.float32).reshape(total_rows, KVH, HD), positions).astype(jnp.bfloat16)
    value_all = keyval[:, KVH * HD:].reshape(total_rows, KVH, HD)
    group_size = H // KVH
    query_grp = query_rot.reshape(total_rows, KVH, group_size, HD)
    allowed = positions[None, :] <= positions[:, None]

    def one_group(operands):
        q_block, k_block, v_block = operands
        scores = jnp.einsum('rgd,sd->grs', q_block.astype(jnp.float32), k_block.astype(jnp.float32)) * HD ** (-0.5)
        scores = jnp.where(allowed[None, :, :], scores, -1e+30)
        row_peak = lax.optimization_barrier(jnp.max(scores, axis=-1, keepdims=True))
        expo = jnp.exp(scores - row_peak)
        prob_rows = (expo / lax.optimization_barrier(jnp.sum(expo, axis=-1, keepdims=True))).astype(jnp.bfloat16)
        mixed = jnp.einsum('grs,sd->rgd', prob_rows.astype(jnp.float32), v_block.astype(jnp.float32))
        return mixed.astype(jnp.bfloat16)
    attended = lax.map(one_group, (jnp.transpose(query_grp, (1, 0, 2, 3)), jnp.transpose(key_rot, (1, 0, 2)), jnp.transpose(value_all, (1, 0, 2))))
    attended = jnp.transpose(attended, (1, 0, 2, 3)).reshape(total_rows, H * HD)
    head_sum = jnp.dot(attended, w_out, preferred_element_type=jnp.float32)
    mid_rows = (tokens_in.astype(jnp.float32) + head_sum).astype(jnp.bfloat16)
    normed_mlp = rms_scale(mid_rows, gain_mlp)
    gate_sum = jnp.dot(normed_mlp, w_gate, preferred_element_type=jnp.float32)
    up_sum = jnp.dot(normed_mlp, w_up, preferred_element_type=jnp.float32)
    hidden = (jax.nn.silu(gate_sum) * up_sum).astype(jnp.bfloat16)
    down_sum = jnp.dot(hidden, w_down, preferred_element_type=jnp.float32)
    return (mid_rows.astype(jnp.float32) + down_sum).astype(jnp.bfloat16)
```

```python
import jax
import jax.numpy as jnp
from jax import lax
from jax.experimental import pallas as pl
from jax.experimental.pallas import tpu as pltpu
from jax.sharding import PartitionSpec as P

H = 64
KVH = 8
HD = 128
EPS = 1e-05
THETA = 10000.0
CHUNKS = 4
PARTS = 2
MESH = pl.DeviceIdType.MESH
F32 = jnp.float32
BF16 = jnp.bfloat16
VMEM = pl.BlockSpec(memory_space=pltpu.VMEM)
ANY = pl.BlockSpec(memory_space=pl.ANY)


def greet(peers):
    barrier = pltpu.get_barrier_semaphore()
    for peer in peers:
        pl.semaphore_signal(barrier, inc=1, device_id=peer, device_id_type=MESH)
    pl.semaphore_wait(barrier, len(peers))


def push(src, dst, sems, slot, device):
    return pltpu.make_async_remote_copy(
        src_ref=src,
        dst_ref=dst,
        send_sem=sems.at[0, slot],
        recv_sem=sems.at[1, slot],
        device_id=device,
        device_id_type=MESH,
    )


def others(axis):
    size = lax.axis_size(axis)
    me = lax.axis_index(axis)
    return [(step, lax.rem(me + step, size), lax.rem(me + size - step, size)) for step in range(1, size)]


def gather_group(out, at, sem_t, sem_s, on_block=lambda section, tensor, order: None):
    section, tensor = lax.axis_index("section"), lax.axis_index("tensor")
    sections, tensors = others("section"), others("tensor")
    size_t = lax.axis_size("tensor")
    started = []

    def pass_on(block_t, slot):
        for step, to, _ in sections:
            block = out.at[at(section, block_t)]
            copy = push(block, block, sem_s, slot * len(sections) + step - 1, {"section": to})
            copy.start()
            started.append(copy)

    for step, to, _ in tensors:
        block = out.at[at(section, tensor)]
        copy = push(block, block, sem_t, step - 1, {"tensor": to})
        copy.start()
        started.append(copy)
    pass_on(tensor, 0)
    on_block(section, tensor, 0)

    def from_sections(slot):
        for step, to, source in sections:
            source_t = lax.rem(tensor + size_t - slot, size_t)
            block = out.at[at(source, source_t)]
            push(block, block, sem_s, slot * len(sections) + step - 1, {"section": to}).wait_recv()
            on_block(source, source_t, (slot + 1) * len(sections) + slot + step - 1)

    for step, to, source in tensors:
        if step == 1:
            from_sections(0)
        block = out.at[at(section, source)]
        push(block, block, sem_t, step - 1, {"tensor": to}).wait_recv()
        pass_on(source, step)
        on_block(section, source, step * (len(sections) + 1))
        if step > 1:
            from_sections(step - 1)
    from_sections(size_t - 1)
    for copy in started:
        copy.wait_send()


def group_peers():
    return [{"tensor": to} for _, to, _ in others("tensor")] + [
        {"section": to} for _, to, _ in others("section")
    ]


def dma_sems(count):
    return pltpu.SemaphoreType.DMA((2, max(1, count)))


def block_order():
    section, tensor = lax.axis_index("section"), lax.axis_index("tensor")
    size_t = lax.axis_size("tensor")

    def from_sections(slot):
        return [(source, lax.rem(tensor + size_t - slot, size_t)) for _, _, source in others("section")]

    order = [(section, tensor)] + from_sections(0)
    for step, _, source in others("tensor"):
        order.append((section, source))
        if step > 1:
            order += from_sections(step - 1)
    return order + from_sections(size_t - 1)


def front_body(
    x_ref, gain_ref, cos_ref, sin_ref, wq_hbm, wk_hbm, att_ref, full_ref,
    blocks, wq, wk, qacc, kacc, stat, kv_src, kv_dst,
    sem_w, sem_own, sem_t, sem_s, sem_kv, sem_kv_out,
):
    section, tensor, me = lax.axis_index("section"), lax.axis_index("tensor"), lax.axis_index("dp")
    size_s, size_t, size_d = lax.axis_size("section"), lax.axis_size("tensor"), lax.axis_size("dp")
    count = size_s * size_t
    index = section * size_t + tensor
    local_rows, width = x_ref.shape
    features = count * width
    heads_dev = qacc.shape[1] // HD
    group_size = H // KVH
    units, _, unit = kv_src.shape
    pieces = HD // unit
    rep = group_size // heads_dev

    order = block_order()
    loads = []
    for k, (s, t) in enumerate(order):
        rows = pl.ds(pl.multiple_of((s * size_t + t) * width, width), width)
        loads.append(
            (
                pltpu.make_async_copy(wq_hbm.at[rows], wq.at[k], sem_w.at[0, k]),
                pltpu.make_async_copy(wk_hbm.at[rows], wk.at[k], sem_w.at[1, k]),
            )
        )
    for pair in loads:
        for load in pair:
            load.start()
    own = pltpu.make_async_copy(x_ref, blocks.at[index], sem_own)
    own.start()

    dps = others("dp")
    everyone = []
    for hop_s in range(size_s):
        for hop_t in range(size_t):
            for hop_d in range(size_d):
                if hop_s + hop_t + hop_d:
                    everyone.append(
                        {
                            "section": lax.rem(section + hop_s, size_s),
                            "tensor": lax.rem(tensor + hop_t, size_t),
                            "dp": lax.rem(me + hop_d, size_d),
                        }
                    )
    greet(everyone)
    own.wait()

    seen = []

    def on_block(s, t, _):
        k = len(seen)
        seen.append(k)
        for load in loads[k]:
            load.wait()
        at = s * size_t + t
        raw = blocks[at]
        full_ref[:, pl.ds(pl.multiple_of(at * width, width), width)] = raw
        rows = raw.astype(F32)
        part = jnp.sum(rows * rows, axis=-1, keepdims=True)
        stat[...] = part if k == 0 else stat[...] + part
        scaled = (rows * gain_ref[at].astype(F32)).astype(BF16)
        tile = tile_of(qacc.shape[1], 256)

        @pl.loop(0, qacc.shape[1] // tile)
        def _(j):
            cols = pl.ds(pl.multiple_of(j * tile, tile), tile)
            term = jnp.dot(scaled, wq[k, :, cols], preferred_element_type=F32)
            qacc[:, cols] = term if k == 0 else qacc[:, cols] + term

        term = jnp.dot(scaled, wk[k], preferred_element_type=F32)
        kacc[...] = term if k == 0 else kacc[...] + term

    gather_group(blocks, lambda s, t: s * size_t + t, sem_t, sem_s, on_block)
    factor = lax.rsqrt(stat[...] * (1.0 / features) + EPS)

    for i in range(units):
        kv_src[i] = (kacc[:, i * unit : (i + 1) * unit] * factor).astype(BF16)

    def dp_rows(at):
        return pl.ds(pl.multiple_of(at * local_rows, local_rows), local_rows)

    half = KVH * pieces

    def kv_copy(i, r, g, kind, piece, step, to):
        return pltpu.make_async_remote_copy(
            src_ref=kv_src.at[i],
            dst_ref=kv_dst.at[kind, piece, dp_rows(me)],
            send_sem=sem_kv_out.at[(i * rep + r) * size_d + step],
            recv_sem=sem_kv.at[1, (kind * pieces + piece) * size_d + step],
            device_id={"section": g // size_t, "tensor": lax.rem(g, size_t), "dp": to},
            device_id_type=MESH,
        )

    hops = [(step, to, source) for step, to, source in dps] + [(0, me, me)]

    def each_send(act):
        for i in range(units):
            u = index * units + i
            kind, piece = u // half, lax.rem(u, pieces)
            head = lax.rem(u, half) // pieces
            for r in range(rep):
                g = head * rep + r
                for step, to, _ in hops:
                    if step:
                        act(kv_copy(i, r, g, kind, piece, step, to), i, kind, piece, False)
                    else:
                        @pl.when(g != index)
                        def _():
                            act(kv_copy(i, r, g, kind, piece, step, to), i, kind, piece, False)

                        @pl.when(g == index)
                        def _():
                            act(None, i, kind, piece, True)

    def begin(copy, i, kind, piece, local):
        if local:
            kv_dst[kind, piece, dp_rows(me), :] = kv_src[i]
        else:
            copy.start()

    each_send(begin)

    cosine, sine = cos_ref[dp_rows(me), :], sin_ref[dp_rows(me), :]
    queries = []
    for h in range(heads_dev):
        q = qacc[:, h * HD : (h + 1) * HD] * factor
        q = q * cosine + pltpu.roll(q, HD // 2, axis=1) * sine
        queries.append(q.astype(BF16))

    head = index // rep
    for kind in range(2):
        for piece in range(pieces):
            g = (kind * half + head * pieces + piece) // units
            for step, to, source in hops:
                dst = kv_dst.at[kind, piece, dp_rows(source)]
                wait = push(dst, dst, sem_kv, (kind * pieces + piece) * size_d + step, {"tensor": tensor})
                if step:
                    wait.wait_recv()
                else:
                    @pl.when(g != index)
                    def _():
                        wait.wait_recv()

    def whole(kind):
        return jnp.concatenate([kv_dst[kind, piece] for piece in range(pieces)], axis=1) if pieces > 1 else kv_dst[kind, 0]

    keys = whole(0).astype(F32)
    keys = (keys * cos_ref[...] + pltpu.roll(keys, HD // 2, axis=1) * sin_ref[...]).astype(BF16)
    values = whole(1)
    total_rows = keys.shape[0]
    block = total_rows // count
    sub = block // PARTS
    shape = (local_rows, total_rows)
    allowed = lax.broadcasted_iota(jnp.int32, shape, 1) <= (
        lax.broadcasted_iota(jnp.int32, shape, 0) + me * local_rows
    )
    for h in range(heads_dev):
        scores = lax.dot_general(
            queries[h], keys, (((1,), (1,)), ((), ())), preferred_element_type=F32
        ) * HD ** (-0.5)
        scores = jnp.where(allowed, scores, -1e30)
        expo = jnp.exp(scores - jnp.max(scores, axis=-1, keepdims=True))
        probs = (expo / jnp.sum(expo, axis=-1, keepdims=True)).astype(BF16)
        mixed = jnp.dot(probs, values, preferred_element_type=F32).astype(BF16)
        for k in range(PARTS):
            for j in range(local_rows // block):
                att_ref[k, j * sub : (j + 1) * sub, h * HD : (h + 1) * HD] = mixed[j * block + k * sub :][:sub]

    def end(copy, i, kind, piece, local):
        if not local:
            copy.wait_send()

    each_send(end)


def front(tokens, gain, cosine, sine, w_query, w_keyval, collective_id):
    size_s, size_t, size_d = lax.axis_size("section"), lax.axis_size("tensor"), lax.axis_size("dp")
    count = size_s * size_t
    local_rows, width = tokens.shape
    kv_cols = w_keyval.shape[1]
    unit = min(kv_cols, HD)
    pieces = HD // unit
    rep = (H // KVH) // (w_query.shape[1] // HD)
    arrivals = 2 * pieces * size_d
    return pl.pallas_call(
        front_body,
        out_shape=(
            jax.ShapeDtypeStruct((PARTS, local_rows // PARTS, w_query.shape[1]), BF16),
            jax.ShapeDtypeStruct((local_rows, count * width), BF16),
        ),
        in_specs=[VMEM, VMEM, VMEM, VMEM, ANY, ANY],
        out_specs=(VMEM, VMEM),
        scratch_shapes=[
            pltpu.VMEM((count, local_rows, width), BF16),
            pltpu.VMEM((count, width, w_query.shape[1]), BF16),
            pltpu.VMEM((count, width, kv_cols), BF16),
            pltpu.VMEM((local_rows, w_query.shape[1]), F32),
            pltpu.VMEM((local_rows, kv_cols), F32),
            pltpu.VMEM((local_rows, 1), F32),
            pltpu.VMEM((kv_cols // unit, local_rows, unit), BF16),
            pltpu.VMEM((2, pieces, local_rows * size_d, unit), BF16),
            pltpu.SemaphoreType.DMA((2, count)),
            pltpu.SemaphoreType.DMA,
            dma_sems(size_t - 1),
            dma_sems(size_t * (size_s - 1)),
            dma_sems(arrivals),
            pltpu.SemaphoreType.DMA((kv_cols // unit * rep * size_d,)),
        ],
        compiler_params=pltpu.CompilerParams(
            collective_id=collective_id, has_side_effects=True, vmem_limit_bytes=66000000
        ),
    )(tokens, gain, cosine, sine, w_query, w_keyval)


def tile_of(width, most):
    return width if width <= most else most


def back_body(
    att_ref, rows_ref, gain_ref, wo_hbm, wg_hbm, wu_hbm, wd_hbm, out_ref,
    wo, wg, wu, wd, att_all, part, pair_rx, comb, z_rx, resid, mid, stat_tx, stat_rx,
    nrm, gu, rx1, tx2, rx2, hid, acc, part2, pair_rx2, comb2, z_rx2,
    sem_w, sem_att, sem_res, sem_p, sem_z, sem_stat, sem_up, sem_dn, sem_s,
    sem_1, sem_2, sem_h, sem_p2, sem_z2,
):
    section, tensor, me = lax.axis_index("section"), lax.axis_index("tensor"), lax.axis_index("dp")
    size_t, size_d = lax.axis_size("tensor"), lax.axis_size("dp")
    group_index = section * size_t + tensor
    parts, dp_sub, width = att_ref.shape
    local_rows = parts * dp_sub
    features = rows_ref.shape[1]
    _, sub, cols = mid.shape
    block = parts * sub
    chunks = gu.shape[1]
    dps, sections, tensors = others("dp"), others("section"), others("tensor")
    hops_s = len(sections)
    sends = []

    loads = [
        pltpu.make_async_copy(wo_hbm.at[:, pl.ds(pl.multiple_of(me * cols, cols), cols)], wo, sem_w.at[0]),
        pltpu.make_async_copy(wg_hbm, wg, sem_w.at[1]),
        pltpu.make_async_copy(wu_hbm, wu, sem_w.at[2]),
        pltpu.make_async_copy(wd_hbm, wd, sem_w.at[3]),
    ]
    for load in loads:
        load.start()

    greet(group_peers() + [{"dp": to} for _, to, _ in dps])

    def send(copy):
        copy.start()
        sends.append(copy)

    def dp_rows(index):
        return pl.ds(pl.multiple_of(index * dp_sub, dp_sub), dp_sub)

    def group_rows(s, t):
        return pl.ds(pl.multiple_of((s * size_t + t) * sub, sub), sub)

    def att_copy(k, step, to):
        return push(att_ref.at[k], att_all.at[k, dp_rows(me)], sem_att, k * (size_d - 1) + step - 1, {"dp": to})

    for k in range(parts):
        for step, to, _ in dps:
            send(att_copy(k, step, to))

    per = local_rows // block
    holder = group_index // per
    held_rows = pl.ds(pl.multiple_of(lax.rem(group_index, per) * block, block), block)

    def resid_copy(step, to):
        src = rows_ref.at[held_rows, pl.ds(pl.multiple_of(to * cols, cols), cols)]
        return push(src, resid, sem_res, step - 1, {"dp": to})

    @pl.when(me == holder)
    def _():
        for step, to, _ in dps:
            resid_copy(step, to).start()
        resid[...] = rows_ref[held_rows, pl.ds(pl.multiple_of(me * cols, cols), cols)]

    for k in range(parts):
        att_all[k, dp_rows(me), :] = att_ref[k]
    loads[0].wait()
    tile = tile_of(cols, 256)

    def pair_copy(k, source, rx, sem, hop, other, step, to):
        return push(
            source.at[k, group_rows(other, to)],
            rx.at[k, hop - 1, step],
            sem,
            (k * hops_s + hop - 1) * size_t + step,
            {"section": other},
        )

    def pair_start(k, source, rx, sem):
        for step, to in [(step, to) for step, to, _ in tensors] + [(0, tensor)]:
            for hop, other, _ in sections:
                send(pair_copy(k, source, rx, sem, hop, other, step, to))

    def paired(k, source, rx, sem, step, to):
        total = source[k, group_rows(section, to), :].astype(F32)
        for hop, other, _ in sections:
            pair_copy(k, source, rx, sem, hop, other, step, to).wait_recv()
            total = total + rx[k, hop - 1, step].astype(F32)
        return total

    def z_copy(k, out, rx, sem, step, to):
        return push(out.at[k, step - 1], rx.at[k, step - 1], sem, k * (size_t - 1) + step - 1, {"tensor": to})

    def z_start(k, source, rx, sem, out, z_in, sem_out):
        for step, to, _ in tensors:
            out[k, step - 1] = paired(k, source, rx, sem, step, to).astype(BF16)
            send(z_copy(k, out, z_in, sem_out, step, to))

    def z_total(k, source, rx, sem, out, z_in, sem_out):
        total = paired(k, source, rx, sem, 0, tensor)
        for step, to, _ in tensors:
            z_copy(k, out, z_in, sem_out, step, to).wait_recv()
            total = total + z_in[k, step - 1].astype(F32)
        return total

    first_set = (part, pair_rx, sem_p)
    last_set = (part2, pair_rx2, sem_p2)

    def head_out(k):
        for step, to, _ in dps:
            att_copy(k, step, to).wait_recv()

        @pl.loop(0, cols // tile)
        def _(j):
            at = pl.ds(pl.multiple_of(j * tile, tile), tile)
            part[k, :, at] = jnp.dot(att_all[k], wo[:, at], preferred_element_type=F32).astype(BF16)

        pair_start(k, *first_set)

    def head_z(k):
        z_start(k, *first_set, comb, z_rx, sem_z)

    def up(k, b):
        at = nrm.at[k, group_rows(section, b)]
        return push(at, at, sem_up, k * size_t + b, {"tensor": lax.rem(tensor + 1, size_t)})

    def down(k, b):
        at = nrm.at[k, group_rows(section, b)]
        return push(at, at, sem_dn, k * size_t + b, {"tensor": lax.rem(tensor + size_t - 1, size_t)})

    def across(k, s, b, hop, other):
        at = nrm.at[k, group_rows(s, b)]
        return push(at, at, sem_s, (k * size_t + b) * hops_s + hop - 1, {"section": other})

    def share_block(k, b):
        for hop, other, _ in sections:
            across(k, section, b, hop, other).start()

    def middle(k):
        summed = z_total(k, *first_set, comb, z_rx, sem_z)
        if k == 0:
            for step, to, source in dps:
                @pl.when(source == holder)
                def _():
                    resid_copy(step, to).wait_recv()

        rows = (resid[k * sub : (k + 1) * sub].astype(F32) + summed).astype(BF16)
        mid[k] = rows
        squares = rows.astype(F32)
        stat = jnp.sum(squares * squares, axis=-1, keepdims=True)
        stat_tx[k] = jnp.broadcast_to(stat, stat_tx.shape[1:])

        def stat_copy(step, to):
            return push(stat_tx.at[k], stat_rx.at[k, step - 1], sem_stat, k * (size_d - 1) + step - 1, {"dp": to})

        for step, to, _ in dps:
            send(stat_copy(step, to))
        for step, to, _ in dps:
            stat_copy(step, to).wait_recv()
            stat = stat + stat_rx[k, step - 1][:, :1]
        factor = lax.rsqrt(stat * (1.0 / features) + EPS)
        nrm[k, group_rows(section, tensor), :] = (
            mid[k].astype(F32) * factor * gain_ref[...].astype(F32)
        ).astype(BF16)

        @pl.when(tensor < size_t - 1)
        def _():
            up(k, tensor).start()

        @pl.when(tensor > 0)
        def _():
            down(k, tensor).start()

        share_block(k, tensor)

    def relay(k, far):
        @pl.when(tensor >= far)
        def _():
            b = tensor - far
            up(k, b).wait_recv()

            @pl.when(tensor < size_t - 1)
            def _():
                up(k, b).start()

            share_block(k, b)

        @pl.when(tensor + far < size_t)
        def _():
            b = tensor + far
            down(k, b).wait_recv()

            @pl.when(tensor > 0)
            def _():
                down(k, b).start()

            share_block(k, b)

    def gathered(k):
        for b in range(size_t):
            for hop, other, source in sections:
                across(k, source, b, hop, other).wait_recv()

    share = gu.shape[3] // 2
    gtile = tile_of(share, 256)
    square = size_d == 4
    if square:
        x, y = lax.rem(me, 2), me // 2
        near = [y * 2 + (1 - x), (1 - y) * 2 + x]
        far_peer = (1 - y) * 2 + (1 - x)
    slots = 2 if square else size_d - 1
    hid_slots = size_d - 1

    def first_copy(k, c, slot, owner, to):
        return push(
            gu.at[k, c, dp_rows(owner)], rx1.at[k, c, slot], sem_1, (k * chunks + c) * slots + slot, {"dp": to}
        )

    def second_copy(k, c, to):
        return push(tx2.at[k, c], rx2.at[k, c], sem_2, k * chunks + c, {"dp": to})

    def hid_copy(k, c, owner, slot, to):
        at = hid.at[k, c, dp_rows(owner)]
        return push(at, at, sem_h, (k * chunks + c) * hid_slots + slot, {"dp": to})

    def gate_up(k):
        if k == 0:
            loads[1].wait()
            loads[2].wait()
        for c in range(chunks):
            @pl.loop(0, share // gtile)
            def _(j):
                src = pl.ds(pl.multiple_of(c * share + j * gtile, gtile), gtile)
                lo = pl.ds(pl.multiple_of(j * gtile, gtile), gtile)
                hi = pl.ds(pl.multiple_of(share + j * gtile, gtile), gtile)
                gu[k, c, :, lo] = jnp.dot(nrm[k], wg[:, src], preferred_element_type=F32).astype(BF16)
                gu[k, c, :, hi] = jnp.dot(nrm[k], wu[:, src], preferred_element_type=F32).astype(BF16)

            if square:
                first = near[c % 2]
                send(first_copy(k, c, 1, far_peer, first))
                send(first_copy(k, c, 0, first, first))
            else:
                for step, to, _ in dps:
                    send(first_copy(k, c, step - 1, to, to))

    def second(k, c):
        if square:
            one, two = near[c % 2], near[1 - c % 2]
            first_copy(k, c, 1, far_peer, one).wait_recv()
            tx2[k, c] = (gu[k, c, dp_rows(two), :].astype(F32) + rx1[k, c, 1].astype(F32)).astype(BF16)
            send(second_copy(k, c, two))

    def hidden(k, c):
        both = gu[k, c, dp_rows(me), :].astype(F32)
        if square:
            one, two = near[c % 2], near[1 - c % 2]
            first_copy(k, c, 0, one, one).wait_recv()
            second_copy(k, c, two).wait_recv()
            both = both + rx1[k, c, 0].astype(F32) + rx2[k, c].astype(F32)
        else:
            for step, to, _ in dps:
                first_copy(k, c, step - 1, to, to).wait_recv()
                both = both + rx1[k, c, step - 1].astype(F32)
        gate, upper = both[:, :share], both[:, share:]
        hid[k, c, dp_rows(me), :] = (gate / (1.0 + jnp.exp(-gate)) * upper).astype(BF16)
        targets = list(enumerate(near)) if square else [(step - 1, to) for step, to, _ in dps]
        for slot, to in targets:
            send(hid_copy(k, c, me, slot, to))

    def pass_hidden(k, c):
        if square:
            one, two = c % 2, 1 - c % 2
            hid_copy(k, c, near[one], one, near[one]).wait_recv()
            send(hid_copy(k, c, near[one], 2, near[two]))

    def down_part(k, c):
        if k == 0 and c == 0:
            loads[3].wait()
        if square:
            two = 1 - c % 2
            arrivals = [(two, near[two]), (2, far_peer)]
        else:
            arrivals = [(step - 1, source) for step, _, source in dps]
        for slot, source in arrivals:
            hid_copy(k, c, source, slot, source).wait_recv()

        @pl.loop(0, cols // tile)
        def _(j):
            at = pl.ds(pl.multiple_of(j * tile, tile), tile)
            term = jnp.dot(hid[k, c], wd[c * share : (c + 1) * share, at], preferred_element_type=F32)
            if c > 0:
                term = acc[:, at] + term
            if c < chunks - 1:
                acc[:, at] = term
            else:
                part2[k, :, at] = term.astype(BF16)

        if c == chunks - 1:
            pair_start(k, *last_set)

    def down_z(k):
        z_start(k, *last_set, comb2, z_rx2, sem_z2)

    def finish(k):
        total = z_total(k, *last_set, comb2, z_rx2, sem_z2)
        out_ref[k * sub : (k + 1) * sub, :] = (mid[k].astype(F32) + total).astype(BF16)

    def each(act, k):
        return [(act, k, c) for c in range(chunks)]

    relays = [[(relay, k, far) for far in range(1, size_t)] for k in range(parts)]
    plan = [(head_out, 0), (head_z, 0)]
    if parts == 2:
        plan += [(head_out, 1), (middle, 0), *relays[0][:2], (head_z, 1), *relays[0][2:], (gathered, 0)]
        plan += [(gate_up, 0), *each(second, 0)[: chunks // 2], (middle, 1), *each(second, 0)[chunks // 2 :]]
        plan += [*relays[1][:2], *each(hidden, 0), *relays[1][2:], (gathered, 1), (gate_up, 1)]
        plan += [*each(second, 1), *each(pass_hidden, 0), *each(hidden, 1), *each(down_part, 0), (down_z, 0)]
        plan += [*each(pass_hidden, 1), *each(down_part, 1), (down_z, 1), (finish, 0), (finish, 1)]
    for act, *at in plan:
        act(*at)

    for copy in sends:
        copy.wait_send()
    for k in range(parts):
        for b in range(size_t):
            @pl.when((tensor >= b) & (tensor < size_t - 1))
            def _():
                up(k, b).wait_send()

            @pl.when((tensor <= b) & (tensor > 0))
            def _():
                down(k, b).wait_send()

            for hop, other, _ in sections:
                across(k, section, b, hop, other).wait_send()

    @pl.when(me == holder)
    def _():
        for step, to, _ in dps:
            resid_copy(step, to).wait_send()


def back(attended, full_rows, gain, w_out, w_gate, w_up, w_down, collective_id):
    size_s, size_t, size_d = lax.axis_size("section"), lax.axis_size("tensor"), lax.axis_size("dp")
    parts, dp_sub, width = attended.shape
    rows = dp_sub * size_d
    sub = rows // (size_s * size_t)
    cols, wide = w_gate.shape
    chunks = min(CHUNKS, wide // 128)
    share = wide // chunks
    slots = 2 if size_d == 4 else size_d - 1
    scatter = [
        pltpu.VMEM((parts, rows, cols), BF16),
        pltpu.VMEM((parts, size_s - 1, size_t, sub, cols), BF16),
        pltpu.VMEM((parts, size_t - 1, sub, cols), BF16),
        pltpu.VMEM((parts, size_t - 1, sub, cols), BF16),
    ]
    return pl.pallas_call(
        back_body,
        out_shape=jax.ShapeDtypeStruct((parts * sub, cols), BF16),
        in_specs=[VMEM, VMEM, VMEM, ANY, ANY, ANY, ANY],
        out_specs=VMEM,
        scratch_shapes=[
            pltpu.VMEM((width, cols), BF16),
            pltpu.VMEM(w_gate.shape, BF16),
            pltpu.VMEM(w_up.shape, BF16),
            pltpu.VMEM(w_down.shape, BF16),
            pltpu.VMEM((parts, rows, width), BF16),
            *scatter,
            pltpu.VMEM((parts * sub, cols), BF16),
            pltpu.VMEM((parts, sub, cols), BF16),
            pltpu.VMEM((parts, sub, 128), F32),
            pltpu.VMEM((parts, size_d - 1, sub, 128), F32),
            pltpu.VMEM((parts, rows, cols), BF16),
            pltpu.VMEM((parts, chunks, rows, 2 * share), BF16),
            pltpu.VMEM((parts, chunks, slots, dp_sub, 2 * share), BF16),
            pltpu.VMEM((parts, chunks, dp_sub, 2 * share), BF16),
            pltpu.VMEM((parts, chunks, dp_sub, 2 * share), BF16),
            pltpu.VMEM((parts, chunks, rows, share), BF16),
            pltpu.VMEM((rows, cols), F32),
            *scatter,
            pltpu.SemaphoreType.DMA((4,)),
            dma_sems(parts * (size_d - 1)),
            dma_sems(size_d - 1),
            dma_sems(parts * (size_s - 1) * size_t),
            dma_sems(parts * (size_t - 1)),
            dma_sems(parts * (size_d - 1)),
            dma_sems(parts * size_t),
            dma_sems(parts * size_t),
            dma_sems(parts * size_t * (size_s - 1)),
            dma_sems(parts * chunks * slots),
            dma_sems(parts * chunks),
            dma_sems(parts * chunks * (size_d - 1)),
            dma_sems(parts * (size_s - 1) * size_t),
            dma_sems(parts * (size_t - 1)),
        ],
        compiler_params=pltpu.CompilerParams(
            collective_id=collective_id, has_side_effects=True, vmem_limit_bytes=66000000
        ),
    )(attended, full_rows, gain, w_out, w_gate, w_up, w_down)


def shards(tokens_in, gain_attn, w_query, w_keyval, w_out, gain_mlp, w_gate, w_up, w_down):
    data_index = lax.axis_index("dp")
    local_rows, width = tokens_in.shape
    total_rows = local_rows * lax.axis_size("dp")
    half_dim = HD // 2
    frequency = THETA ** (-jnp.arange(half_dim, dtype=jnp.float32) * 2.0 / HD)
    angles = jnp.arange(total_rows, dtype=jnp.int32).astype(F32)[:, None] * frequency[None, :]
    cosine, sine = jnp.cos(angles), jnp.sin(angles)
    attended, full_rows = front(
        tokens_in,
        gain_attn.reshape(-1, 1, width),
        jnp.concatenate([cosine, cosine], axis=1),
        jnp.concatenate([-sine, sine], axis=1),
        w_query,
        w_keyval,
        1,
    )
    cols = w_gate.shape[0]
    gain = lax.dynamic_slice_in_dim(gain_mlp, data_index * cols, cols, 0)[None, :]
    return back(attended, full_rows, gain, w_out, w_gate, w_up, w_down, 2)


def solution(mesh):
    placed = (
        P("dp", ("section", "tensor")),
        P(),
        P(None, ("section", "tensor")),
        P(None, ("section", "tensor")),
        P(("section", "tensor"), None),
        P(),
        P("dp", ("section", "tensor")),
        P("dp", ("section", "tensor")),
        P(("section", "tensor"), "dp"),
    )
    return jax.shard_map(
        shards,
        mesh=mesh,
        in_specs=placed,
        out_specs=P(("section", "tensor"), "dp"),
        check_vma=False,
    )
```

```python
import jax
import jax.numpy as jnp
from jax import lax
from jax.experimental import pallas as pl
from jax.experimental.pallas import tpu as pltpu
from jax.sharding import PartitionSpec as P

H = 64
KVH = 8
HD = 128
EPS = 1e-05
THETA = 10000.0
CHUNKS = 2
TILE = 1024
GTILE = 512
PIECES = 2
MESH = pl.DeviceIdType.MESH
F32 = jnp.float32
BF16 = jnp.bfloat16
VMEM = pl.BlockSpec(memory_space=pltpu.VMEM)
ANY = pl.BlockSpec(memory_space=pl.ANY)


def greet(peers):
    barrier = pltpu.get_barrier_semaphore()
    for peer in peers:
        pl.semaphore_signal(barrier, inc=1, device_id=peer, device_id_type=MESH)
    pl.semaphore_wait(barrier, len(peers))


def push(src, dst, sems, slot, device):
    return pltpu.make_async_remote_copy(
        src_ref=src,
        dst_ref=dst,
        send_sem=sems.at[0, slot],
        recv_sem=sems.at[1, slot],
        device_id=device,
        device_id_type=MESH,
    )


def others(axis):
    size = lax.axis_size(axis)
    me = lax.axis_index(axis)
    return [(step, lax.rem(me + step, size), lax.rem(me + size - step, size)) for step in range(1, size)]


def z_routes():
    tensor, size_t = lax.axis_index("tensor"), lax.axis_size("tensor")
    if size_t == 4:
        flip, swap = tensor + 1 - 2 * lax.rem(tensor, 2), lax.rem(tensor + 2, 4)
        return [(1, swap), (0, flip)], [(0, flip, None), (1, swap, (2, flip)), (2, 3 - tensor, None)]
    hops = others("tensor")
    return [(step - 1, to) for step, to, _ in hops], [(step - 1, source, None) for step, _, source in hops]


def gather_group(out, sem_t, sem_s, on_block):
    section, tensor = lax.axis_index("section"), lax.axis_index("tensor")
    sections = others("section")
    size_t = lax.axis_size("tensor")
    piece = out.shape[1] // PIECES
    z_sends, z_arrivals = z_routes()
    started = []

    def begin(copy):
        copy.start()
        started.append(copy)

    def z_copy(slot, b, p, to):
        rows = out.at[section * size_t + b, pl.ds(p * piece, piece)]
        return push(rows, rows, sem_t, slot * PIECES + p, {"tensor": to})

    def s_copy(slot, s, b, step, to):
        block = out.at[s * size_t + b]
        return push(block, block, sem_s, slot * len(sections) + step - 1, {"section": to})

    def pass_on(slot, b):
        for step, to, _ in sections:
            begin(s_copy(slot, section, b, step, to))

    for slot, to in z_sends:
        for p in range(PIECES):
            begin(z_copy(slot, tensor, p, to))
    pass_on(size_t - 1, tensor)
    on_block(section, tensor)

    def from_sections(slot, b):
        for step, to, source in sections:
            s_copy(slot, source, b, step, to).wait_recv()
            on_block(source, b)

    late = [(size_t - 1, tensor)]
    for slot, source, onward in z_arrivals:
        for p in range(PIECES):
            z_copy(slot, source, p, source).wait_recv()
            if onward:
                begin(z_copy(onward[0], source, p, onward[1]))
        pass_on(slot, source)
        from_sections(*late.pop())
        on_block(section, source)
        late.append((slot, source))
    from_sections(*late.pop())
    for copy in started:
        copy.wait_send()


def group_peers():
    return [{"tensor": to} for _, to, _ in others("tensor")] + [
        {"section": to} for _, to, _ in others("section")
    ]


def dma_sems(count):
    return pltpu.SemaphoreType.DMA((2, max(1, count)))


def block_order():
    section, tensor = lax.axis_index("section"), lax.axis_index("tensor")
    order, late = [(section, tensor)], tensor
    for _, b, _ in z_routes()[1]:
        order += [(source, late) for _, _, source in others("section")] + [(section, b)]
        late = b
    return order + [(source, late) for _, _, source in others("section")]


def parts_of(block):
    return max(1, block // 16)


def front_body(
    x_ref, gain_ref, cos_ref, sin_ref, wq_hbm, wk_hbm, att_ref, full_ref,
    blocks, wq, wk, qacc, kacc, stat, kv_src, kv_dst,
    sem_w, sem_own, sem_t, sem_s, sem_kv, sem_kv_out,
):
    section, tensor, me = lax.axis_index("section"), lax.axis_index("tensor"), lax.axis_index("dp")
    size_s, size_t, size_d = lax.axis_size("section"), lax.axis_size("tensor"), lax.axis_size("dp")
    count = size_s * size_t
    index = section * size_t + tensor
    local_rows, width = x_ref.shape
    features = count * width
    heads_dev = qacc.shape[1] // HD
    group_size = H // KVH
    units, _, unit = kv_src.shape
    pieces = HD // unit
    rep = group_size // heads_dev

    order = block_order()
    loads = []
    for k, (s, t) in enumerate(order):
        rows = pl.ds(pl.multiple_of((s * size_t + t) * width, width), width)
        loads.append(
            (
                pltpu.make_async_copy(wq_hbm.at[rows], wq.at[k], sem_w.at[0, k]),
                pltpu.make_async_copy(wk_hbm.at[rows], wk.at[k], sem_w.at[1, k]),
            )
        )
    for pair in loads:
        for load in pair:
            load.start()
    own = pltpu.make_async_copy(x_ref, blocks.at[index], sem_own)
    own.start()

    dps = others("dp")
    everyone = []
    for hop_s in range(size_s):
        for hop_t in range(size_t):
            for hop_d in range(size_d):
                if hop_s + hop_t + hop_d:
                    everyone.append(
                        {
                            "section": lax.rem(section + hop_s, size_s),
                            "tensor": lax.rem(tensor + hop_t, size_t),
                            "dp": lax.rem(me + hop_d, size_d),
                        }
                    )
    greet(everyone)
    own.wait()

    seen = []

    def on_block(s, t):
        k = len(seen)
        seen.append(k)
        for load in loads[k]:
            load.wait()
        at = s * size_t + t
        raw = blocks[at]
        full_ref[:, pl.ds(pl.multiple_of(at * width, width), width)] = raw
        rows = raw.astype(F32)
        part = jnp.sum(rows * rows, axis=-1, keepdims=True)
        stat[...] = part if k == 0 else stat[...] + part
        scaled = (rows * gain_ref[at].astype(F32)).astype(BF16)
        tile = tile_of(qacc.shape[1], 256)

        @pl.loop(0, qacc.shape[1] // tile)
        def _(j):
            cols = pl.ds(pl.multiple_of(j * tile, tile), tile)
            term = jnp.dot(scaled, wq[k, :, cols], preferred_element_type=F32)
            qacc[:, cols] = term if k == 0 else qacc[:, cols] + term

        term = jnp.dot(scaled, wk[k], preferred_element_type=F32)
        kacc[...] = term if k == 0 else kacc[...] + term

    gather_group(blocks, sem_t, sem_s, on_block)
    factor = lax.rsqrt(stat[...] * (1.0 / features) + EPS)

    for i in range(units):
        kv_src[i] = (kacc[:, i * unit : (i + 1) * unit] * factor).astype(BF16)

    def dp_rows(at):
        return pl.ds(pl.multiple_of(at * local_rows, local_rows), local_rows)

    half = KVH * pieces

    def kv_copy(i, r, g, kind, piece, step, to):
        return pltpu.make_async_remote_copy(
            src_ref=kv_src.at[i],
            dst_ref=kv_dst.at[kind, piece, dp_rows(me)],
            send_sem=sem_kv_out.at[(i * rep + r) * size_d + step],
            recv_sem=sem_kv.at[1, (kind * pieces + piece) * size_d + step],
            device_id={"section": g // size_t, "tensor": lax.rem(g, size_t), "dp": to},
            device_id_type=MESH,
        )

    hops = [(step, to, source) for step, to, source in dps] + [(0, me, me)]

    def each_send(act):
        for i in range(units):
            u = index * units + i
            kind, piece = u // half, lax.rem(u, pieces)
            head = lax.rem(u, half) // pieces
            for r in range(rep):
                g = head * rep + r
                for step, to, _ in hops:
                    if step:
                        act(kv_copy(i, r, g, kind, piece, step, to), i, kind, piece, False)
                    else:
                        @pl.when(g != index)
                        def _():
                            act(kv_copy(i, r, g, kind, piece, step, to), i, kind, piece, False)

                        @pl.when(g == index)
                        def _():
                            act(None, i, kind, piece, True)

    def begin(copy, i, kind, piece, local):
        if local:
            kv_dst[kind, piece, dp_rows(me), :] = kv_src[i]
        else:
            copy.start()

    each_send(begin)

    cosine, sine = cos_ref[dp_rows(me), :], sin_ref[dp_rows(me), :]
    queries = []
    for h in range(heads_dev):
        q = qacc[:, h * HD : (h + 1) * HD] * factor
        q = q * cosine + pltpu.roll(q, HD // 2, axis=1) * sine
        queries.append(q.astype(BF16))

    head = index // rep
    for kind in range(2):
        for piece in range(pieces):
            g = (kind * half + head * pieces + piece) // units
            for step, to, source in hops:
                dst = kv_dst.at[kind, piece, dp_rows(source)]
                wait = push(dst, dst, sem_kv, (kind * pieces + piece) * size_d + step, {"tensor": tensor})
                if step:
                    wait.wait_recv()
                else:
                    @pl.when(g != index)
                    def _():
                        wait.wait_recv()

    def whole(kind):
        return jnp.concatenate([kv_dst[kind, piece] for piece in range(pieces)], axis=1) if pieces > 1 else kv_dst[kind, 0]

    keys = whole(0).astype(F32)
    keys = (keys * cos_ref[...] + pltpu.roll(keys, HD // 2, axis=1) * sin_ref[...]).astype(BF16)
    values = whole(1)
    total_rows = keys.shape[0]
    block = total_rows // count
    parts = parts_of(block)
    sub = block // parts
    shape = (local_rows, total_rows)
    allowed = lax.broadcasted_iota(jnp.int32, shape, 1) <= (
        lax.broadcasted_iota(jnp.int32, shape, 0) + me * local_rows
    )
    for h in range(heads_dev):
        scores = lax.dot_general(
            queries[h], keys, (((1,), (1,)), ((), ())), preferred_element_type=F32
        ) * HD ** (-0.5)
        scores = jnp.where(allowed, scores, -1e30)
        expo = jnp.exp(scores - jnp.max(scores, axis=-1, keepdims=True))
        probs = (expo / jnp.sum(expo, axis=-1, keepdims=True)).astype(BF16)
        mixed = jnp.dot(probs, values, preferred_element_type=F32).astype(BF16)
        for k in range(parts):
            for j in range(local_rows // block):
                att_ref[k, j * sub : (j + 1) * sub, h * HD : (h + 1) * HD] = mixed[j * block + k * sub :][:sub]

    def end(copy, i, kind, piece, local):
        if not local:
            copy.wait_send()

    each_send(end)


def front(tokens, gain, cosine, sine, w_query, w_keyval, collective_id):
    size_s, size_t, size_d = lax.axis_size("section"), lax.axis_size("tensor"), lax.axis_size("dp")
    count = size_s * size_t
    local_rows, width = tokens.shape
    kv_cols = w_keyval.shape[1]
    unit = min(kv_cols, HD)
    pieces = HD // unit
    rep = (H // KVH) // (w_query.shape[1] // HD)
    arrivals = 2 * pieces * size_d
    parts = parts_of(local_rows * size_d // count)
    return pl.pallas_call(
        front_body,
        out_shape=(
            jax.ShapeDtypeStruct((parts, local_rows // parts, w_query.shape[1]), BF16),
            jax.ShapeDtypeStruct((local_rows, count * width), BF16),
        ),
        in_specs=[VMEM, VMEM, VMEM, VMEM, ANY, ANY],
        out_specs=(VMEM, VMEM),
        scratch_shapes=[
            pltpu.VMEM((count, local_rows, width), BF16),
            pltpu.VMEM((count, width, w_query.shape[1]), BF16),
            pltpu.VMEM((count, width, kv_cols), BF16),
            pltpu.VMEM((local_rows, w_query.shape[1]), F32),
            pltpu.VMEM((local_rows, kv_cols), F32),
            pltpu.VMEM((local_rows, 1), F32),
            pltpu.VMEM((kv_cols // unit, local_rows, unit), BF16),
            pltpu.VMEM((2, pieces, local_rows * size_d, unit), BF16),
            pltpu.SemaphoreType.DMA((2, count)),
            pltpu.SemaphoreType.DMA,
            dma_sems((size_t - 1) * PIECES),
            dma_sems(size_t * (size_s - 1)),
            dma_sems(arrivals),
            pltpu.SemaphoreType.DMA((kv_cols // unit * rep * size_d,)),
        ],
        compiler_params=pltpu.CompilerParams(
            collective_id=collective_id, has_side_effects=True, vmem_limit_bytes=66000000
        ),
    )(tokens, gain, cosine, sine, w_query, w_keyval)


def tile_of(width, most):
    return width if width <= most else most


def back_body(
    att_ref, rows_ref, gain_ref, wo_hbm, wg_hbm, wu_hbm, wd_hbm, out_ref,
    wo, wg, wu, wd, att_all, part, pair_rx, comb, z_rx, resid, stat_tx, stat_rx,
    nrm, scaled, gu, rx1, tx2, rx2, hid, part2, pair_rx2, comb2, z_rx2,
    sem_w, sem_att, sem_res, sem_p, sem_z, sem_stat, sem_t, sem_s,
    sem_1, sem_2, sem_h, sem_p2, sem_z2,
):
    section, tensor, me = lax.axis_index("section"), lax.axis_index("tensor"), lax.axis_index("dp")
    size_t, size_d = lax.axis_size("tensor"), lax.axis_size("dp")
    group_index = section * size_t + tensor
    parts, dp_sub, width = att_ref.shape
    local_rows = parts * dp_sub
    features = rows_ref.shape[1]
    block, cols = resid.shape
    sub = block // parts
    chunks = gu.shape[1]
    dps, sections, tensors = others("dp"), others("section"), others("tensor")
    hops_s = len(sections)
    sends = []

    loads = [
        pltpu.make_async_copy(wo_hbm.at[:, pl.ds(pl.multiple_of(me * cols, cols), cols)], wo, sem_w.at[0]),
        pltpu.make_async_copy(wg_hbm, wg, sem_w.at[1]),
        pltpu.make_async_copy(wu_hbm, wu, sem_w.at[2]),
        pltpu.make_async_copy(wd_hbm, wd, sem_w.at[3]),
    ]
    loads[0].start()

    greet(group_peers() + [{"dp": to} for _, to, _ in dps])

    def send(copy):
        copy.start()
        sends.append(copy)

    def dp_rows(index):
        return pl.ds(pl.multiple_of(index * dp_sub, dp_sub), dp_sub)

    def group_rows(s, t):
        return pl.ds(pl.multiple_of((s * size_t + t) * sub, sub), sub)

    def att_copy(k, step, to):
        return push(att_ref.at[k], att_all.at[k, dp_rows(me)], sem_att, k * (size_d - 1) + step - 1, {"dp": to})

    def att_start(k):
        for step, to, _ in dps:
            if k < parts:
                send(att_copy(k, step, to))

    att_start(0)
    per = local_rows // block
    holder = group_index // per
    held_rows = pl.ds(pl.multiple_of(lax.rem(group_index, per) * block, block), block)

    def resid_copy(step, to):
        src = rows_ref.at[held_rows, pl.ds(pl.multiple_of(to * cols, cols), cols)]
        return push(src, resid, sem_res, step - 1, {"dp": to})

    loads[0].wait()
    att_start(1)
    for load in loads[1:]:
        load.start()

    @pl.when(me == holder)
    def _():
        for step, to, _ in dps:
            resid_copy(step, to).start()
        resid[...] = rows_ref[held_rows, pl.ds(pl.multiple_of(me * cols, cols), cols)]

    for k in range(parts):
        att_all[k, dp_rows(me), :] = att_ref[k]
    tile = tile_of(cols, TILE)

    def pair_copy(k, source, rx, sem, hop, other, step, to):
        return push(
            source.at[k, group_rows(other, to)],
            rx.at[k, hop - 1, step],
            sem,
            (k * hops_s + hop - 1) * size_t + step,
            {"section": other},
        )

    def pair_start(k, source, rx, sem):
        for step, to in [(step, to) for step, to, _ in tensors] + [(0, tensor)]:
            for hop, other, _ in sections:
                send(pair_copy(k, source, rx, sem, hop, other, step, to))

    def paired(k, source, rx, sem, step, to):
        total = source[k, group_rows(section, to), :].astype(F32)
        for hop, other, _ in sections:
            pair_copy(k, source, rx, sem, hop, other, step, to).wait_recv()
            total = total + rx[k, hop - 1, step].astype(F32)
        return total

    def z_copy(k, out, rx, sem, step, to):
        return push(out.at[k, step - 1], rx.at[k, step - 1], sem, k * (size_t - 1) + step - 1, {"tensor": to})

    def z_start(k, source, rx, sem, out, z_in, sem_out):
        for step, to, _ in tensors:
            out[k, step - 1] = paired(k, source, rx, sem, step, to).astype(BF16)
            send(z_copy(k, out, z_in, sem_out, step, to))

    def z_total(k, source, rx, sem, out, z_in, sem_out):
        total = paired(k, source, rx, sem, 0, tensor)
        for step, to, _ in tensors:
            z_copy(k, out, z_in, sem_out, step, to).wait_recv()
            total = total + z_in[k, step - 1].astype(F32)
        return total

    first_set = (part, pair_rx, sem_p)
    last_set = (part2, pair_rx2, sem_p2)

    def head_out(k):
        for step, to, _ in dps:
            att_copy(k, step, to).wait_recv()
        att_start(k + 2)

        @pl.loop(0, cols // tile)
        def _(j):
            at = pl.ds(pl.multiple_of(j * tile, tile), tile)
            part[k, :, at] = jnp.dot(att_all[k], wo[:, at], preferred_element_type=F32).astype(BF16)

        pair_start(k, *first_set)

    def head_z(k):
        z_start(k, *first_set, comb, z_rx, sem_z)

    z_sends, z_arrivals = z_routes()

    def pass_copy(k, slot, b, to):
        at = nrm.at[k, group_rows(section, b)]
        return push(at, at, sem_t, k * (size_t - 1) + slot, {"tensor": to})

    def across(k, s, b, slot, hop, other):
        at = nrm.at[k, group_rows(s, b)]
        return push(at, at, sem_s, (k * size_t + slot) * hops_s + hop - 1, {"section": other})

    def share_block(k, b, slot):
        for hop, other, _ in sections:
            send(across(k, section, b, slot, hop, other))

    def middle(k):
        summed = z_total(k, *first_set, comb, z_rx, sem_z)
        if k == 0:
            for step, to, source in dps:
                @pl.when(source == holder)
                def _():
                    resid_copy(step, to).wait_recv()

        rows = (resid[k * sub : (k + 1) * sub].astype(F32) + summed).astype(BF16)
        nrm[k, group_rows(section, tensor), :] = rows
        for slot, to in z_sends:
            send(pass_copy(k, slot, tensor, to))
        share_block(k, tensor, size_t - 1)

    def relay(k):
        for slot, source, onward in z_arrivals:
            pass_copy(k, slot, source, source).wait_recv()
            if onward:
                send(pass_copy(k, onward[0], source, onward[1]))
            share_block(k, source, slot)

    def gathered(k):
        for slot, b in [(size_t - 1, tensor)] + [(slot, source) for slot, source, _ in z_arrivals]:
            for hop, other, source in sections:
                across(k, source, b, slot, hop, other).wait_recv()

    def stat_copy(k, step, to):
        return push(
            stat_tx.at[k, dp_rows(to)], stat_rx.at[k, step - 1], sem_stat, k * (size_d - 1) + step - 1, {"dp": to}
        )

    def scale(k):
        @pl.loop(0, stat_tx.shape[1] // 16)
        def _(j):
            at = pl.ds(pl.multiple_of(j * 16, 16), 16)
            rows = nrm[k, at, :].astype(F32)
            stat = jnp.sum(rows * rows, axis=-1, keepdims=True)
            stat_tx[k, at, :] = jnp.broadcast_to(stat, (16, 128))
            scaled[at, :] = (rows * gain_ref[...].astype(F32)).astype(BF16)

        for step, to, _ in dps:
            send(stat_copy(k, step, to))

    factors = {}

    def factor_of(k):
        if k not in factors:
            stat = stat_tx[k, dp_rows(me), :][:, :1]
            for step, to, _ in dps:
                stat_copy(k, step, to).wait_recv()
                stat = stat + stat_rx[k, step - 1][:, :1]
            factors[k] = lax.rsqrt(stat * (1.0 / features) + EPS)
        return factors[k]

    share = gu.shape[3] // 2
    gtile = tile_of(share, GTILE)
    square = size_d == 4
    if square:
        x, y = lax.rem(me, 2), me // 2
        near = [y * 2 + (1 - x), (1 - y) * 2 + x]
        far_peer = (1 - y) * 2 + (1 - x)
    slots = 2 if square else size_d - 1
    hid_slots = size_d - 1

    def first_copy(k, c, slot, owner, to):
        return push(
            gu.at[k, c, dp_rows(owner)], rx1.at[k, c, slot], sem_1, (k * chunks + c) * slots + slot, {"dp": to}
        )

    def second_copy(k, c, to):
        return push(tx2.at[k, c], rx2.at[k, c], sem_2, k * chunks + c, {"dp": to})

    def hid_copy(k, c, owner, slot, to):
        at = hid.at[k, c, dp_rows(owner)]
        return push(at, at, sem_h, (k * chunks + c) * hid_slots + slot, {"dp": to})

    def gate_up(k):
        if k == 0:
            loads[1].wait()
            loads[2].wait()
        scale(k)
        for c in range(chunks):
            @pl.loop(0, share // gtile)
            def _(j):
                src = pl.ds(pl.multiple_of(c * share + j * gtile, gtile), gtile)
                lo = pl.ds(pl.multiple_of(j * gtile, gtile), gtile)
                hi = pl.ds(pl.multiple_of(share + j * gtile, gtile), gtile)
                gu[k, c, :, lo] = jnp.dot(scaled[...], wg[:, src], preferred_element_type=F32).astype(BF16)
                gu[k, c, :, hi] = jnp.dot(scaled[...], wu[:, src], preferred_element_type=F32).astype(BF16)

            if square:
                first = near[c % 2]
                send(first_copy(k, c, 1, far_peer, first))
                send(first_copy(k, c, 0, first, first))
            else:
                for step, to, _ in dps:
                    send(first_copy(k, c, step - 1, to, to))

    def second(k, c):
        if square:
            one, two = near[c % 2], near[1 - c % 2]
            first_copy(k, c, 1, far_peer, one).wait_recv()
            tx2[k, c] = (gu[k, c, dp_rows(two), :].astype(F32) + rx1[k, c, 1].astype(F32)).astype(BF16)
            send(second_copy(k, c, two))

    def hidden(k, c):
        both = gu[k, c, dp_rows(me), :].astype(F32)
        if square:
            one, two = near[c % 2], near[1 - c % 2]
            first_copy(k, c, 0, one, one).wait_recv()
            second_copy(k, c, two).wait_recv()
            both = both + rx1[k, c, 0].astype(F32) + rx2[k, c].astype(F32)
        else:
            for step, to, _ in dps:
                first_copy(k, c, step - 1, to, to).wait_recv()
                both = both + rx1[k, c, step - 1].astype(F32)
        both = both * factor_of(k)
        gate, upper = both[:, :share], both[:, share:]
        hid[k, c, dp_rows(me), :] = (gate / (1.0 + jnp.exp(-gate)) * upper).astype(BF16)
        targets = list(enumerate(near)) if square else [(step - 1, to) for step, to, _ in dps]
        for slot, to in targets:
            send(hid_copy(k, c, me, slot, to))

    def pass_hidden(k, c):
        if square:
            one, two = c % 2, 1 - c % 2
            hid_copy(k, c, near[one], one, near[one]).wait_recv()
            send(hid_copy(k, c, near[one], 2, near[two]))

    def down_wait(k, c):
        if k == 0 and c == 0:
            loads[3].wait()
        if square:
            two = 1 - c % 2
            arrivals = [(two, near[two]), (2, far_peer)]
        else:
            arrivals = [(step - 1, source) for step, _, source in dps]
        for slot, source in arrivals:
            hid_copy(k, c, source, slot, source).wait_recv()

    def down_out(k):
        @pl.loop(0, cols // tile)
        def _(j):
            at = pl.ds(pl.multiple_of(j * tile, tile), tile)
            term = jnp.dot(hid[k, 0], wd[:share, at], preferred_element_type=F32)
            for c in range(1, chunks):
                term = term + jnp.dot(hid[k, c], wd[c * share : (c + 1) * share, at], preferred_element_type=F32)
            part2[k, :, at] = term.astype(BF16)

        pair_start(k, *last_set)

    def down_z(k):
        z_start(k, *last_set, comb2, z_rx2, sem_z2)

    def finish(k):
        total = z_total(k, *last_set, comb2, z_rx2, sem_z2)
        out_ref[k * sub : (k + 1) * sub, :] = (nrm[k, group_rows(section, tensor), :].astype(F32) + total).astype(BF16)

    def each(act, k):
        return [(act, k, c) for c in range(chunks)]

    plan = [(head_out, 0), (head_z, 0)]
    if parts > 1:
        plan += [(head_out, 1), (head_z, 1)]
    plan += [(middle, 0)]
    if parts > 2:
        plan += [(head_out, 2)]
    plan += [(relay, 0), (gathered, 0)]
    for k in range(parts):
        if k + 1 < parts:
            plan += [(middle, k + 1)]
        if k + 2 < parts:
            plan += [(head_z, k + 2)]
        plan += [(gate_up, k)]
        if k > 0:
            plan += [*each(pass_hidden, k - 1)]
        if k + 1 < parts:
            plan += [(relay, k + 1)]
        if k + 3 < parts:
            plan += [(head_out, k + 3)]
        plan += [*each(second, k)]
        if k > 0:
            plan += [*each(down_wait, k - 1), (down_out, k - 1), (down_z, k - 1)]
        plan += [*each(hidden, k)]
        if k > 1:
            plan += [(finish, k - 2)]
        if k + 1 < parts:
            plan += [(gathered, k + 1)]
    last = parts - 1
    plan += [*each(pass_hidden, last), *each(down_wait, last), (down_out, last), (down_z, last)]
    plan += [(finish, k) for k in range(max(0, parts - 2), parts)]
    for act, *at in plan:
        act(*at)

    for copy in sends:
        copy.wait_send()
    @pl.when(me == holder)
    def _():
        for step, to, _ in dps:
            resid_copy(step, to).wait_send()


def back(attended, full_rows, gain, w_out, w_gate, w_up, w_down, collective_id):
    size_s, size_t, size_d = lax.axis_size("section"), lax.axis_size("tensor"), lax.axis_size("dp")
    parts, dp_sub, width = attended.shape
    rows = dp_sub * size_d
    sub = rows // (size_s * size_t)
    cols, wide = w_gate.shape
    chunks = min(CHUNKS, wide // 128)
    share = wide // chunks
    slots = 2 if size_d == 4 else size_d - 1
    scatter = [
        pltpu.VMEM((parts, rows, cols), BF16),
        pltpu.VMEM((parts, size_s - 1, size_t, sub, cols), BF16),
        pltpu.VMEM((parts, size_t - 1, sub, cols), BF16),
        pltpu.VMEM((parts, size_t - 1, sub, cols), BF16),
    ]
    return pl.pallas_call(
        back_body,
        out_shape=jax.ShapeDtypeStruct((parts * sub, cols), BF16),
        in_specs=[VMEM, VMEM, VMEM, ANY, ANY, ANY, ANY],
        out_specs=VMEM,
        scratch_shapes=[
            pltpu.VMEM((width, cols), BF16),
            pltpu.VMEM(w_gate.shape, BF16),
            pltpu.VMEM(w_up.shape, BF16),
            pltpu.VMEM(w_down.shape, BF16),
            pltpu.VMEM((parts, rows, width), BF16),
            *scatter,
            pltpu.VMEM((parts * sub, cols), BF16),
            pltpu.VMEM((parts, rows, 128), F32),
            pltpu.VMEM((parts, size_d - 1, dp_sub, 128), F32),
            pltpu.VMEM((parts, rows, cols), BF16),
            pltpu.VMEM((rows, cols), BF16),
            pltpu.VMEM((parts, chunks, rows, 2 * share), BF16),
            pltpu.VMEM((parts, chunks, slots, dp_sub, 2 * share), BF16),
            pltpu.VMEM((parts, chunks, dp_sub, 2 * share), BF16),
            pltpu.VMEM((parts, chunks, dp_sub, 2 * share), BF16),
            pltpu.VMEM((parts, chunks, rows, share), BF16),
            *scatter,
            pltpu.SemaphoreType.DMA((4,)),
            dma_sems(parts * (size_d - 1)),
            dma_sems(size_d - 1),
            dma_sems(parts * (size_s - 1) * size_t),
            dma_sems(parts * (size_t - 1)),
            dma_sems(parts * (size_d - 1)),
            dma_sems(parts * (size_t - 1)),
            dma_sems(parts * size_t * (size_s - 1)),
            dma_sems(parts * chunks * slots),
            dma_sems(parts * chunks),
            dma_sems(parts * chunks * (size_d - 1)),
            dma_sems(parts * (size_s - 1) * size_t),
            dma_sems(parts * (size_t - 1)),
        ],
        compiler_params=pltpu.CompilerParams(
            collective_id=collective_id, has_side_effects=True, vmem_limit_bytes=66000000
        ),
    )(attended, full_rows, gain, w_out, w_gate, w_up, w_down)


def shards(tokens_in, gain_attn, w_query, w_keyval, w_out, gain_mlp, w_gate, w_up, w_down):
    data_index = lax.axis_index("dp")
    local_rows, width = tokens_in.shape
    total_rows = local_rows * lax.axis_size("dp")
    half_dim = HD // 2
    frequency = THETA ** (-jnp.arange(half_dim, dtype=jnp.float32) * 2.0 / HD)
    angles = jnp.arange(total_rows, dtype=jnp.int32).astype(F32)[:, None] * frequency[None, :]
    cosine, sine = jnp.cos(angles), jnp.sin(angles)
    attended, full_rows = front(
        tokens_in,
        gain_attn.reshape(-1, 1, width),
        jnp.concatenate([cosine, cosine], axis=1),
        jnp.concatenate([-sine, sine], axis=1),
        w_query,
        w_keyval,
        1,
    )
    cols = w_gate.shape[0]
    gain = lax.dynamic_slice_in_dim(gain_mlp, data_index * cols, cols, 0)[None, :]
    return back(attended, full_rows, gain, w_out, w_gate, w_up, w_down, 2)


def solution(mesh):
    placed = (
        P("dp", ("section", "tensor")),
        P(),
        P(None, ("section", "tensor")),
        P(None, ("section", "tensor")),
        P(("section", "tensor"), None),
        P(),
        P("dp", ("section", "tensor")),
        P("dp", ("section", "tensor")),
        P(("section", "tensor"), "dp"),
    )
    return jax.shard_map(
        shards,
        mesh=mesh,
        in_specs=placed,
        out_specs=P(("section", "tensor"), "dp"),
        check_vma=False,
    )
```

```python
import jax
import jax.numpy as jnp
import numpy as np
from jax import lax
from jax.experimental import pallas as pl
from jax.experimental.pallas import tpu as pltpu
from jax.sharding import PartitionSpec as P

H = 64
KVH = 8
HD = 128
EPS = 1e-05
THETA = 10000.0
CHUNKS = 2
TILE = 1024
GTILE = 512
PIECES = 2
ORDER = (
    "H0 Z0 H1 Z1",
    "M0 H2 M1 R0",
    "G0 Z2 U0 H3",
    "R1 G1 Z3 U1",
    "S0 M2 M3 S1",
    "R2 G2 U2 D0",
    "R3 G3 U3 D1",
    "S2 P0 S3 D2",
    "P1 D3 V0 W0",
    "Y0 P2 V1 W1",
    "Y1 P3 F0 V2",
    "W2 Y2 F1 V3",
    "W3 Y3 F2 F3",
)
MESH = pl.DeviceIdType.MESH
F32 = jnp.float32
BF16 = jnp.bfloat16
VMEM = pl.BlockSpec(memory_space=pltpu.VMEM)
ANY = pl.BlockSpec(memory_space=pl.ANY)


def greet(peers):
    barrier = pltpu.get_barrier_semaphore()
    for peer in peers:
        pl.semaphore_signal(barrier, inc=1, device_id=peer, device_id_type=MESH)
    pl.semaphore_wait(barrier, len(peers))


def push(src, dst, sems, slot, device):
    return pltpu.make_async_remote_copy(
        src_ref=src,
        dst_ref=dst,
        send_sem=sems.at[0, slot],
        recv_sem=sems.at[1, slot],
        device_id=device,
        device_id_type=MESH,
    )


def others(axis):
    size = lax.axis_size(axis)
    me = lax.axis_index(axis)
    return [(step, lax.rem(me + step, size), lax.rem(me + size - step, size)) for step in range(1, size)]


def z_routes():
    hops = others("tensor")
    return [(step - 1, to) for step, to, _ in hops], [(step - 1, source, None) for step, _, source in hops]


def gather_group(out, sem_t, sem_s, on_block):
    section, tensor = lax.axis_index("section"), lax.axis_index("tensor")
    sections = others("section")
    size_t = lax.axis_size("tensor")
    piece = out.shape[1] // PIECES
    line = size_t == 4
    started = []

    def begin(copy):
        copy.start()
        started.append(copy)

    def z_copy(b, p, to, slot):
        rows = out.at[section * size_t + b, pl.ds(p * piece, piece)]
        return pltpu.make_async_remote_copy(
            src_ref=rows,
            dst_ref=rows,
            send_sem=sem_t.at[0, slot * PIECES + p],
            recv_sem=sem_t.at[1, (b if line else slot) * PIECES + p],
            device_id={"tensor": to},
            device_id_type=MESH,
        )

    def s_copy(slot, s, b, step, to):
        block = out.at[s * size_t + b]
        return push(block, block, sem_s, slot * len(sections) + step - 1, {"section": to})

    def pass_on(slot, b):
        for step, to, _ in sections:
            begin(s_copy(slot, section, b, step, to))

    def from_sections(slot, b):
        for step, to, source in sections:
            s_copy(slot, source, b, step, to).wait_recv()
            on_block(source, b)

    above, below = lax.rem(tensor + 1, size_t), lax.rem(tensor + size_t - 1, size_t)

    def line_up(p, b, act):
        @pl.when((b <= tensor) & (tensor < size_t - 1))
        def _():
            act(z_copy(b, p, above, b))

    def line_down(p, b, slot, act):
        @pl.when((b >= tensor) & (tensor > 0))
        def _():
            act(z_copy(b, p, below, slot))

    def start(copy):
        copy.start()

    def done(copy):
        copy.wait_send()

    sources = near_first()
    for p in range(PIECES):
        if line:
            line_up(p, tensor, start)
            line_down(p, tensor, size_t, start)
        else:
            for step, to, _ in others("tensor"):
                begin(z_copy(tensor, p, to, step - 1))
    pass_on(size_t - 1, tensor)
    on_block(section, tensor)
    from_sections(size_t - 1, tensor)

    def arrive(slot, p):
        source = sources[slot]
        z_copy(source, p, source, slot).wait_recv()
        if line:
            line_up(p, source, start)
            line_down(p, source, source, start)
        if p == PIECES - 1:
            pass_on(slot, source)

    for slot, source in enumerate(sources):
        for p in range(PIECES):
            arrive(slot, p)
            if slot > 0 and p == 0:
                on_block(section, sources[slot - 1])
        if slot > 0:
            from_sections(slot - 1, sources[slot - 1])
    last = len(sources) - 1
    on_block(section, sources[last])
    from_sections(last, sources[last])
    for copy in started:
        copy.wait_send()
    if line:
        for p in range(PIECES):
            line_down(p, tensor, size_t, done)
            for b in [tensor, *sources]:
                line_up(p, b, done)
            for b in sources:
                line_down(p, b, b, done)


def group_peers():
    return [{"tensor": to} for _, to, _ in others("tensor")] + [
        {"section": to} for _, to, _ in others("section")
    ]


def dma_sems(count):
    return pltpu.SemaphoreType.DMA((2, max(1, count)))


def near_first():
    tensor = lax.axis_index("tensor")
    if lax.axis_size("tensor") == 4:
        upper = tensor // 2
        return [tensor + 1 - 2 * lax.rem(tensor, 2), 2 - upper, 3 - 3 * upper]
    return [source for _, _, source in others("tensor")]


def block_order():
    section, tensor = lax.axis_index("section"), lax.axis_index("tensor")
    order = []
    for b in [tensor, *near_first()]:
        order += [(section, b)] + [(source, b) for _, _, source in others("section")]
    return order


def parts_of(block):
    return max(1, block // 16)


def times_gain(rows, gain32, first):
    tiles = range(rows.shape[1] // 128)
    return jnp.concatenate(
        [rows[:, i * 128 : (i + 1) * 128] * gain32[pl.ds(first + i, 1), :] for i in tiles], axis=1
    )


def front_body(
    x_ref, gain_ref, cos_ref, sin_ref, wq_hbm, wk_hbm, att_ref, full_ref,
    gain32, blocks, wq, wk, qacc, kacc, stat, kv_src, kv_dst,
    sem_w, sem_own, sem_t, sem_s, sem_kv, sem_kv_out,
):
    section, tensor, me = lax.axis_index("section"), lax.axis_index("tensor"), lax.axis_index("dp")
    size_s, size_t, size_d = lax.axis_size("section"), lax.axis_size("tensor"), lax.axis_size("dp")
    count = size_s * size_t
    index = section * size_t + tensor
    local_rows, width = x_ref.shape
    features = count * width
    heads_dev = qacc.shape[1] // HD
    group_size = H // KVH
    units, _, unit = kv_src.shape
    pieces = HD // unit
    rep = group_size // heads_dev

    order = block_order()
    loads = []
    for k, (s, t) in enumerate(order):
        rows = pl.ds(pl.multiple_of((s * size_t + t) * width, width), width)
        loads.append(
            (
                pltpu.make_async_copy(wq_hbm.at[rows], wq.at[k], sem_w.at[0, k]),
                pltpu.make_async_copy(wk_hbm.at[rows], wk.at[k], sem_w.at[1, k]),
            )
        )
    for pair in loads:
        for load in pair:
            load.start()
    own = pltpu.make_async_copy(x_ref, blocks.at[index], sem_own)
    own.start()
    gain32[...] = gain_ref[...].astype(F32)

    dps = others("dp")
    everyone = []
    for hop_s in range(size_s):
        for hop_t in range(size_t):
            for hop_d in range(size_d):
                if hop_s + hop_t + hop_d:
                    everyone.append(
                        {
                            "section": lax.rem(section + hop_s, size_s),
                            "tensor": lax.rem(tensor + hop_t, size_t),
                            "dp": lax.rem(me + hop_d, size_d),
                        }
                    )
    greet(everyone)
    own.wait()

    seen = []

    def on_block(s, t):
        k = len(seen)
        seen.append(k)
        for load in loads[k]:
            load.wait()
        at = s * size_t + t
        raw = blocks[at]
        full_ref[:, pl.ds(pl.multiple_of(at * width, width), width)] = raw
        rows = raw.astype(F32)
        part = jnp.sum(rows * rows, axis=-1, keepdims=True)
        stat[...] = part if k == 0 else stat[...] + part
        scaled = times_gain(rows, gain32, at * (width // 128)).astype(BF16)
        tile = tile_of(qacc.shape[1], GTILE)

        @pl.loop(0, qacc.shape[1] // tile)
        def _(j):
            cols = pl.ds(pl.multiple_of(j * tile, tile), tile)
            term = jnp.dot(scaled, wq[k, :, cols], preferred_element_type=F32)
            qacc[:, cols] = term if k == 0 else qacc[:, cols] + term

        term = jnp.dot(scaled, wk[k], preferred_element_type=F32)
        kacc[...] = term if k == 0 else kacc[...] + term

    gather_group(blocks, sem_t, sem_s, on_block)
    factor = lax.rsqrt(stat[...] * (1.0 / features) + EPS)

    for i in range(units):
        kv_src[i] = (kacc[:, i * unit : (i + 1) * unit] * factor).astype(BF16)

    def dp_rows(at):
        return pl.ds(pl.multiple_of(at * local_rows, local_rows), local_rows)

    half = KVH * pieces

    def kv_copy(i, r, g, kind, piece, step, to):
        return pltpu.make_async_remote_copy(
            src_ref=kv_src.at[i],
            dst_ref=kv_dst.at[kind, piece, dp_rows(me)],
            send_sem=sem_kv_out.at[(i * rep + r) * size_d + step],
            recv_sem=sem_kv.at[1, (kind * pieces + piece) * size_d + step],
            device_id={"section": g // size_t, "tensor": lax.rem(g, size_t), "dp": to},
            device_id_type=MESH,
        )

    hops = [(step, to, source) for step, to, source in dps] + [(0, me, me)]

    def each_send(act):
        for i in range(units):
            u = index * units + i
            kind, piece = u // half, lax.rem(u, pieces)
            head = lax.rem(u, half) // pieces
            for r in range(rep):
                g = head * rep + r
                for step, to, _ in hops:
                    if step:
                        act(kv_copy(i, r, g, kind, piece, step, to), i, kind, piece, False)
                    else:
                        @pl.when(g != index)
                        def _():
                            act(kv_copy(i, r, g, kind, piece, step, to), i, kind, piece, False)

                        @pl.when(g == index)
                        def _():
                            act(None, i, kind, piece, True)

    def begin(copy, i, kind, piece, local):
        if local:
            kv_dst[kind, piece, dp_rows(me), :] = kv_src[i]
        else:
            copy.start()

    each_send(begin)

    cosine, sine = cos_ref[dp_rows(me), :], sin_ref[dp_rows(me), :]
    queries = []
    for h in range(heads_dev):
        q = qacc[:, h * HD : (h + 1) * HD] * factor
        q = q * cosine + pltpu.roll(q, HD // 2, axis=1) * sine
        queries.append(q.astype(BF16))

    head = index // rep
    for kind in range(2):
        for piece in range(pieces):
            g = (kind * half + head * pieces + piece) // units
            for step, to, source in hops:
                dst = kv_dst.at[kind, piece, dp_rows(source)]
                wait = push(dst, dst, sem_kv, (kind * pieces + piece) * size_d + step, {"tensor": tensor})
                if step:
                    wait.wait_recv()
                else:
                    @pl.when(g != index)
                    def _():
                        wait.wait_recv()

    def whole(kind):
        return jnp.concatenate([kv_dst[kind, piece] for piece in range(pieces)], axis=1) if pieces > 1 else kv_dst[kind, 0]

    keys = whole(0).astype(F32)
    keys = (keys * cos_ref[...] + pltpu.roll(keys, HD // 2, axis=1) * sin_ref[...]).astype(BF16)
    values = whole(1)
    total_rows = keys.shape[0]
    block = total_rows // count
    parts = parts_of(block)
    sub = block // parts
    shape = (local_rows, total_rows)
    allowed = lax.broadcasted_iota(jnp.int32, shape, 1) <= (
        lax.broadcasted_iota(jnp.int32, shape, 0) + me * local_rows
    )
    for h in range(heads_dev):
        scores = lax.dot_general(
            queries[h], keys, (((1,), (1,)), ((), ())), preferred_element_type=F32
        ) * HD ** (-0.5)
        scores = jnp.where(allowed, scores, -1e30)
        expo = jnp.exp(scores - jnp.max(scores, axis=-1, keepdims=True))
        probs = (expo / jnp.sum(expo, axis=-1, keepdims=True)).astype(BF16)
        mixed = jnp.dot(probs, values, preferred_element_type=F32).astype(BF16)
        for k in range(parts):
            for j in range(local_rows // block):
                att_ref[k, j * sub : (j + 1) * sub, h * HD : (h + 1) * HD] = mixed[j * block + k * sub :][:sub]

    def end(copy, i, kind, piece, local):
        if not local:
            copy.wait_send()

    each_send(end)


def front(tokens, gain, cosine, sine, w_query, w_keyval, collective_id):
    size_s, size_t, size_d = lax.axis_size("section"), lax.axis_size("tensor"), lax.axis_size("dp")
    count = size_s * size_t
    local_rows, width = tokens.shape
    kv_cols = w_keyval.shape[1]
    unit = min(kv_cols, HD)
    pieces = HD // unit
    rep = (H // KVH) // (w_query.shape[1] // HD)
    arrivals = 2 * pieces * size_d
    parts = parts_of(local_rows * size_d // count)
    return pl.pallas_call(
        front_body,
        out_shape=(
            jax.ShapeDtypeStruct((parts, local_rows // parts, w_query.shape[1]), BF16),
            jax.ShapeDtypeStruct((local_rows, count * width), BF16),
        ),
        in_specs=[VMEM, VMEM, VMEM, VMEM, ANY, ANY],
        out_specs=(VMEM, VMEM),
        scratch_shapes=[
            pltpu.VMEM(gain.shape, F32),
            pltpu.VMEM((count, local_rows, width), BF16),
            pltpu.VMEM((count, width, w_query.shape[1]), BF16),
            pltpu.VMEM((count, width, kv_cols), BF16),
            pltpu.VMEM((local_rows, w_query.shape[1]), F32),
            pltpu.VMEM((local_rows, kv_cols), F32),
            pltpu.VMEM((local_rows, 1), F32),
            pltpu.VMEM((kv_cols // unit, local_rows, unit), BF16),
            pltpu.VMEM((2, pieces, local_rows * size_d, unit), BF16),
            pltpu.SemaphoreType.DMA((2, count)),
            pltpu.SemaphoreType.DMA,
            dma_sems((size_t + 1) * PIECES),
            dma_sems(size_t * (size_s - 1)),
            dma_sems(arrivals),
            pltpu.SemaphoreType.DMA((kv_cols // unit * rep * size_d,)),
        ],
        compiler_params=pltpu.CompilerParams(
            collective_id=collective_id, has_side_effects=True, vmem_limit_bytes=66000000
        ),
    )(tokens, gain, cosine, sine, w_query, w_keyval)


def tile_of(width, most):
    return width if width <= most else most


def back_body(
    att_ref, rows_ref, gain_ref, wo_hbm, wg_hbm, wu_hbm, wd_hbm, out_ref,
    gain32, wo, wg, wu, wd, att_all, part, pair_rx, comb, z_rx, resid, stat_tx, stat_rx,
    nrm, scaled, gu, rx1, tx2, rx2, hid, part2, pair_rx2, comb2, z_rx2,
    sem_w, sem_att, sem_res, sem_p, sem_z, sem_stat, sem_t, sem_s,
    sem_1, sem_2, sem_h, sem_p2, sem_z2,
):
    section, tensor, me = lax.axis_index("section"), lax.axis_index("tensor"), lax.axis_index("dp")
    size_t, size_d = lax.axis_size("tensor"), lax.axis_size("dp")
    group_index = section * size_t + tensor
    parts, dp_sub, width = att_ref.shape
    local_rows = parts * dp_sub
    features = rows_ref.shape[1]
    block, cols = resid.shape
    sub = block // parts
    chunks = gu.shape[1]
    dps, sections, tensors = others("dp"), others("section"), others("tensor")
    hops_s = len(sections)
    sends = []

    loads = [
        pltpu.make_async_copy(wo_hbm.at[:, pl.ds(pl.multiple_of(me * cols, cols), cols)], wo, sem_w.at[0]),
        pltpu.make_async_copy(wg_hbm, wg, sem_w.at[1]),
        pltpu.make_async_copy(wu_hbm, wu, sem_w.at[2]),
        pltpu.make_async_copy(wd_hbm, wd, sem_w.at[3]),
    ]
    loads[0].start()
    gain32[...] = gain_ref[...].astype(F32)

    greet(group_peers() + [{"dp": to} for _, to, _ in dps])

    def send(copy):
        copy.start()
        sends.append(copy)

    def dp_rows(index):
        return pl.ds(pl.multiple_of(index * dp_sub, dp_sub), dp_sub)

    def group_rows(s, t):
        return pl.ds(pl.multiple_of((s * size_t + t) * sub, sub), sub)

    def att_copy(k, step, to):
        return push(att_ref.at[k], att_all.at[k, dp_rows(me)], sem_att, k * (size_d - 1) + step - 1, {"dp": to})

    def att_start(k):
        for step, to, _ in dps:
            if k < parts:
                send(att_copy(k, step, to))

    att_start(0)
    per = local_rows // block
    holder = group_index // per
    held_rows = pl.ds(pl.multiple_of(lax.rem(group_index, per) * block, block), block)

    def resid_copy(step, to):
        src = rows_ref.at[held_rows, pl.ds(pl.multiple_of(to * cols, cols), cols)]
        return push(src, resid, sem_res, step - 1, {"dp": to})

    loads[0].wait()
    att_start(1)
    for load in loads[1:]:
        load.start()

    @pl.when(me == holder)
    def _():
        for step, to, _ in dps:
            resid_copy(step, to).start()
        resid[...] = rows_ref[held_rows, pl.ds(pl.multiple_of(me * cols, cols), cols)]

    for k in range(parts):
        att_all[k, dp_rows(me), :] = att_ref[k]
    tile = tile_of(cols, TILE)

    def pair_copy(k, source, rx, sem, hop, other, step, to):
        return push(
            source.at[k, group_rows(other, to)],
            rx.at[k, hop - 1, step],
            sem,
            (k * hops_s + hop - 1) * size_t + step,
            {"section": other},
        )

    def pair_start(k, source, rx, sem):
        for step, to in [(step, to) for step, to, _ in tensors] + [(0, tensor)]:
            for hop, other, _ in sections:
                send(pair_copy(k, source, rx, sem, hop, other, step, to))

    def paired(k, source, rx, sem, step, to):
        total = source[k, group_rows(section, to), :].astype(F32)
        for hop, other, _ in sections:
            pair_copy(k, source, rx, sem, hop, other, step, to).wait_recv()
            total = total + rx[k, hop - 1, step].astype(F32)
        return total

    def z_copy(k, out, rx, sem, step, to):
        return push(out.at[k, step - 1], rx.at[k, step - 1], sem, k * (size_t - 1) + step - 1, {"tensor": to})

    def z_start(k, source, rx, sem, out, z_in, sem_out):
        for step, to, _ in tensors:
            out[k, step - 1] = paired(k, source, rx, sem, step, to).astype(BF16)
            send(z_copy(k, out, z_in, sem_out, step, to))

    def z_total(k, source, rx, sem, out, z_in, sem_out):
        total = paired(k, source, rx, sem, 0, tensor)
        for step, to, _ in tensors:
            z_copy(k, out, z_in, sem_out, step, to).wait_recv()
            total = total + z_in[k, step - 1].astype(F32)
        return total

    first_set = (part, pair_rx, sem_p)
    last_set = (part2, pair_rx2, sem_p2)

    def head_out(k):
        for step, to, _ in dps:
            att_copy(k, step, to).wait_recv()
        att_start(k + 2)

        @pl.loop(0, cols // tile)
        def _(j):
            at = pl.ds(pl.multiple_of(j * tile, tile), tile)
            part[k, :, at] = jnp.dot(att_all[k], wo[:, at], preferred_element_type=F32).astype(BF16)

        pair_start(k, *first_set)

    def head_z(k):
        z_start(k, *first_set, comb, z_rx, sem_z)

    z_sends, z_arrivals = z_routes()

    def pass_copy(k, slot, b, to):
        at = nrm.at[k, group_rows(section, b)]
        return push(at, at, sem_t, k * (size_t - 1) + slot, {"tensor": to})

    def across(k, s, b, slot, hop, other):
        at = nrm.at[k, group_rows(s, b)]
        return push(at, at, sem_s, (k * size_t + slot) * hops_s + hop - 1, {"section": other})

    def share_block(k, b, slot):
        for hop, other, _ in sections:
            send(across(k, section, b, slot, hop, other))

    def middle(k):
        summed = z_total(k, *first_set, comb, z_rx, sem_z)
        if k == 0:
            for step, to, source in dps:
                @pl.when(source == holder)
                def _():
                    resid_copy(step, to).wait_recv()

        rows = (resid[k * sub : (k + 1) * sub].astype(F32) + summed).astype(BF16)
        nrm[k, group_rows(section, tensor), :] = rows
        for slot, to in z_sends:
            send(pass_copy(k, slot, tensor, to))
        share_block(k, tensor, size_t - 1)

    def relay(k):
        for slot, source, onward in z_arrivals:
            pass_copy(k, slot, source, source).wait_recv()
            if onward:
                send(pass_copy(k, onward[0], source, onward[1]))
            share_block(k, source, slot)

    def gathered(k):
        for slot, b in [(size_t - 1, tensor)] + [(slot, source) for slot, source, _ in z_arrivals]:
            for hop, other, source in sections:
                across(k, source, b, slot, hop, other).wait_recv()

    def stat_copy(k, step, to):
        return push(
            stat_tx.at[k, dp_rows(to)], stat_rx.at[k, step - 1], sem_stat, k * (size_d - 1) + step - 1, {"dp": to}
        )

    def scale(k):
        @pl.loop(0, stat_tx.shape[1] // 16)
        def _(j):
            at = pl.ds(pl.multiple_of(j * 16, 16), 16)
            rows = nrm[k, at, :].astype(F32)
            stat = jnp.sum(rows * rows, axis=-1, keepdims=True)
            stat_tx[k, at, :] = jnp.broadcast_to(stat, (16, 128))
            scaled[at, :] = times_gain(rows, gain32, me * (cols // 128)).astype(BF16)

        for step, to, _ in dps:
            send(stat_copy(k, step, to))

    factors = {}

    def factor_of(k):
        if k not in factors:
            stat = stat_tx[k, dp_rows(me), :][:, :1]
            for step, to, _ in dps:
                stat_copy(k, step, to).wait_recv()
                stat = stat + stat_rx[k, step - 1][:, :1]
            factors[k] = lax.rsqrt(stat * (1.0 / features) + EPS)
        return factors[k]

    share = gu.shape[3] // 2
    gtile = tile_of(share, GTILE)
    square = size_d == 4
    if square:
        x, y = lax.rem(me, 2), me // 2
        near = [y * 2 + (1 - x), (1 - y) * 2 + x]
        far_peer = (1 - y) * 2 + (1 - x)
    slots = 2 if square else size_d - 1
    hid_slots = size_d - 1

    def first_copy(k, c, slot, owner, to):
        return push(
            gu.at[k, c, dp_rows(owner)], rx1.at[k, c, slot], sem_1, (k * chunks + c) * slots + slot, {"dp": to}
        )

    def second_copy(k, c, to):
        return push(tx2.at[k, c], rx2.at[k, c], sem_2, k * chunks + c, {"dp": to})

    def hid_copy(k, c, owner, slot, to):
        at = hid.at[k, c, dp_rows(owner)]
        return push(at, at, sem_h, (k * chunks + c) * hid_slots + slot, {"dp": to})

    def gate_up(k):
        if k == 0:
            loads[1].wait()
            loads[2].wait()
        scale(k)
        for c in range(chunks):
            @pl.loop(0, share // gtile)
            def _(j):
                src = pl.ds(pl.multiple_of(c * share + j * gtile, gtile), gtile)
                lo = pl.ds(pl.multiple_of(j * gtile, gtile), gtile)
                hi = pl.ds(pl.multiple_of(share + j * gtile, gtile), gtile)
                gu[k, c, :, lo] = jnp.dot(scaled[...], wg[:, src], preferred_element_type=F32).astype(BF16)
                gu[k, c, :, hi] = jnp.dot(scaled[...], wu[:, src], preferred_element_type=F32).astype(BF16)

            if square:
                first = near[c % 2]
                send(first_copy(k, c, 1, far_peer, first))
                send(first_copy(k, c, 0, first, first))
            else:
                for step, to, _ in dps:
                    send(first_copy(k, c, step - 1, to, to))

    def second(k, c):
        if square:
            one, two = near[c % 2], near[1 - c % 2]
            first_copy(k, c, 1, far_peer, one).wait_recv()
            tx2[k, c] = (gu[k, c, dp_rows(two), :].astype(F32) + rx1[k, c, 1].astype(F32)).astype(BF16)
            send(second_copy(k, c, two))

    def hidden(k, c):
        both = gu[k, c, dp_rows(me), :].astype(F32)
        if square:
            one, two = near[c % 2], near[1 - c % 2]
            first_copy(k, c, 0, one, one).wait_recv()
            second_copy(k, c, two).wait_recv()
            both = both + rx1[k, c, 0].astype(F32) + rx2[k, c].astype(F32)
        else:
            for step, to, _ in dps:
                first_copy(k, c, step - 1, to, to).wait_recv()
                both = both + rx1[k, c, step - 1].astype(F32)
        both = both * factor_of(k)
        gate, upper = both[:, :share], both[:, share:]
        hid[k, c, dp_rows(me), :] = (gate / (1.0 + jnp.exp(-gate)) * upper).astype(BF16)
        targets = list(enumerate(near)) if square else [(step - 1, to) for step, to, _ in dps]
        for slot, to in targets:
            send(hid_copy(k, c, me, slot, to))

    def pass_hidden(k, c):
        if square:
            one, two = c % 2, 1 - c % 2
            hid_copy(k, c, near[one], one, near[one]).wait_recv()
            send(hid_copy(k, c, near[one], 2, near[two]))

    def down_wait(k, c):
        if k == 0 and c == 0:
            loads[3].wait()
        if square:
            two = 1 - c % 2
            arrivals = [(two, near[two]), (2, far_peer)]
        else:
            arrivals = [(step - 1, source) for step, _, source in dps]
        for slot, source in arrivals:
            hid_copy(k, c, source, slot, source).wait_recv()

    def down_out(k):
        @pl.loop(0, cols // tile)
        def _(j):
            at = pl.ds(pl.multiple_of(j * tile, tile), tile)
            term = jnp.dot(hid[k, 0], wd[:share, at], preferred_element_type=F32)
            for c in range(1, chunks):
                term = term + jnp.dot(hid[k, c], wd[c * share : (c + 1) * share, at], preferred_element_type=F32)
            part2[k, :, at] = term.astype(BF16)

        pair_start(k, *last_set)

    def down_z(k):
        z_start(k, *last_set, comb2, z_rx2, sem_z2)

    def finish(k):
        total = z_total(k, *last_set, comb2, z_rx2, sem_z2)
        out_ref[k * sub : (k + 1) * sub, :] = (nrm[k, group_rows(section, tensor), :].astype(F32) + total).astype(BF16)

    def each(act, k):
        return [(act, k, c) for c in range(chunks)]

    def add(act, k):
        if 0 <= k < parts and (act, k) not in added:
            added.append((act, k))
            plan.extend(each(act, k) if act in (second, hidden, pass_hidden, down_wait) else [(act, k)])

    added, plan = [], []
    names = {
        "H": head_out, "Z": head_z, "M": middle, "R": relay, "G": gathered, "U": gate_up, "S": second,
        "D": hidden, "P": pass_hidden, "V": down_wait, "W": down_out, "Y": down_z, "F": finish,
    }
    for line in ORDER:
        for step in line.split():
            add(names[step[0]], int(step[1]))
    for k in range(parts):
        for act in names.values():
            add(act, k)
    for act, *at in plan:
        act(*at)

    for copy in sends:
        copy.wait_send()
    @pl.when(me == holder)
    def _():
        for step, to, _ in dps:
            resid_copy(step, to).wait_send()


def back(attended, full_rows, gain, w_out, w_gate, w_up, w_down, collective_id):
    size_s, size_t, size_d = lax.axis_size("section"), lax.axis_size("tensor"), lax.axis_size("dp")
    parts, dp_sub, width = attended.shape
    rows = dp_sub * size_d
    sub = rows // (size_s * size_t)
    cols, wide = w_gate.shape
    chunks = min(CHUNKS, wide // 128)
    share = wide // chunks
    slots = 2 if size_d == 4 else size_d - 1
    scatter = [
        pltpu.VMEM((parts, rows, cols), BF16),
        pltpu.VMEM((parts, size_s - 1, size_t, sub, cols), BF16),
        pltpu.VMEM((parts, size_t - 1, sub, cols), BF16),
        pltpu.VMEM((parts, size_t - 1, sub, cols), BF16),
    ]
    return pl.pallas_call(
        back_body,
        out_shape=jax.ShapeDtypeStruct((parts * sub, cols), BF16),
        in_specs=[VMEM, VMEM, VMEM, ANY, ANY, ANY, ANY],
        out_specs=VMEM,
        scratch_shapes=[
            pltpu.VMEM(gain.shape, F32),
            pltpu.VMEM((width, cols), BF16),
            pltpu.VMEM(w_gate.shape, BF16),
            pltpu.VMEM(w_up.shape, BF16),
            pltpu.VMEM(w_down.shape, BF16),
            pltpu.VMEM((parts, rows, width), BF16),
            *scatter,
            pltpu.VMEM((parts * sub, cols), BF16),
            pltpu.VMEM((parts, rows, 128), F32),
            pltpu.VMEM((parts, size_d - 1, dp_sub, 128), F32),
            pltpu.VMEM((parts, rows, cols), BF16),
            pltpu.VMEM((rows, cols), BF16),
            pltpu.VMEM((parts, chunks, rows, 2 * share), BF16),
            pltpu.VMEM((parts, chunks, slots, dp_sub, 2 * share), BF16),
            pltpu.VMEM((parts, chunks, dp_sub, 2 * share), BF16),
            pltpu.VMEM((parts, chunks, dp_sub, 2 * share), BF16),
            pltpu.VMEM((parts, chunks, rows, share), BF16),
            *scatter,
            pltpu.SemaphoreType.DMA((4,)),
            dma_sems(parts * (size_d - 1)),
            dma_sems(size_d - 1),
            dma_sems(parts * (size_s - 1) * size_t),
            dma_sems(parts * (size_t - 1)),
            dma_sems(parts * (size_d - 1)),
            dma_sems(parts * (size_t - 1)),
            dma_sems(parts * size_t * (size_s - 1)),
            dma_sems(parts * chunks * slots),
            dma_sems(parts * chunks),
            dma_sems(parts * chunks * (size_d - 1)),
            dma_sems(parts * (size_s - 1) * size_t),
            dma_sems(parts * (size_t - 1)),
        ],
        compiler_params=pltpu.CompilerParams(
            collective_id=collective_id, has_side_effects=True, vmem_limit_bytes=66000000
        ),
    )(attended, full_rows, gain, w_out, w_gate, w_up, w_down)


def shards(tokens_in, gain_attn, w_query, w_keyval, w_out, gain_mlp, w_gate, w_up, w_down):
    local_rows, width = tokens_in.shape
    total_rows = local_rows * lax.axis_size("dp")
    frequency = THETA ** (-np.arange(HD // 2) * 2.0 / HD)
    angles = np.arange(total_rows)[:, None] * frequency[None, :]
    cosine, sine = np.cos(angles), np.sin(angles)
    attended, full_rows = front(
        tokens_in,
        gain_attn.reshape(-1, 128),
        jnp.asarray(np.concatenate([cosine, cosine], axis=1), F32),
        jnp.asarray(np.concatenate([-sine, sine], axis=1), F32),
        w_query,
        w_keyval,
        1,
    )
    return back(attended, full_rows, gain_mlp.reshape(-1, 128), w_out, w_gate, w_up, w_down, 2)


def solution(mesh):
    placed = (
        P("dp", ("section", "tensor")),
        P(),
        P(None, ("section", "tensor")),
        P(None, ("section", "tensor")),
        P(("section", "tensor"), None),
        P(),
        P("dp", ("section", "tensor")),
        P("dp", ("section", "tensor")),
        P(("section", "tensor"), "dp"),
    )
    return jax.shard_map(
        shards,
        mesh=mesh,
        in_specs=placed,
        out_specs=P(("section", "tensor"), "dp"),
        check_vma=False,
    )
```

```python
import jax
import jax.numpy as jnp
import numpy as np
from jax import lax
from jax.experimental import pallas as pl
from jax.experimental.pallas import tpu as pltpu
from jax.sharding import PartitionSpec as P

H = 64
KVH = 8
HD = 128
EPS = 1e-05
THETA = 10000.0
TILE = 1024
GTILE = 512
PIECES = 2
ORDER = (
    "H0 Z0 H1 Z1",
    "M0 H2 M1 R0",
    "G0 Z2 U0 H3",
    "R1 G1 Z3 U1",
    "S0 M2 S1 D0",
    "M3 R2 P0 G2",
    "D1 U2 R3 G3",
    "U3 S2 P1 V0",
    "W0 S3 Y0 D2",
    "D3 P2 V1 W1",
    "Y1 P3 F0 V2",
    "W2 Y2 F1 V3",
    "W3 Y3 F2 F3",
)
MESH = pl.DeviceIdType.MESH
F32 = jnp.float32
BF16 = jnp.bfloat16
VMEM = pl.BlockSpec(memory_space=pltpu.VMEM)
ANY = pl.BlockSpec(memory_space=pl.ANY)


def greet(peers):
    barrier = pltpu.get_barrier_semaphore()
    for peer in peers:
        pl.semaphore_signal(barrier, inc=1, device_id=peer, device_id_type=MESH)
    pl.semaphore_wait(barrier, len(peers))


def push(src, dst, sems, slot, device):
    return pltpu.make_async_remote_copy(
        src_ref=src,
        dst_ref=dst,
        send_sem=sems.at[0, slot],
        recv_sem=sems.at[1, slot],
        device_id=device,
        device_id_type=MESH,
    )


def others(axis):
    size = lax.axis_size(axis)
    me = lax.axis_index(axis)
    return [(step, lax.rem(me + step, size), lax.rem(me + size - step, size)) for step in range(1, size)]


def z_routes():
    hops = others("tensor")
    return [(step - 1, to) for step, to, _ in hops], [(step - 1, source, None) for step, _, source in hops]


def gather_group(out, sem_t, sem_s, on_block):
    section, tensor = lax.axis_index("section"), lax.axis_index("tensor")
    sections = others("section")
    size_t = lax.axis_size("tensor")
    piece = out.shape[1] // PIECES
    line = size_t == 4
    started = []

    def begin(copy):
        copy.start()
        started.append(copy)

    def z_copy(b, p, to, slot):
        rows = out.at[section * size_t + b, pl.ds(p * piece, piece)]
        return pltpu.make_async_remote_copy(
            src_ref=rows,
            dst_ref=rows,
            send_sem=sem_t.at[0, slot * PIECES + p],
            recv_sem=sem_t.at[1, (b if line else slot) * PIECES + p],
            device_id={"tensor": to},
            device_id_type=MESH,
        )

    def s_copy(slot, s, b, step, to):
        block = out.at[s * size_t + b]
        return push(block, block, sem_s, slot * len(sections) + step - 1, {"section": to})

    def pass_on(slot, b):
        for step, to, _ in sections:
            begin(s_copy(slot, section, b, step, to))

    def from_sections(slot, b):
        for step, to, source in sections:
            s_copy(slot, source, b, step, to).wait_recv()
            on_block(source, b)

    above, below = lax.rem(tensor + 1, size_t), lax.rem(tensor + size_t - 1, size_t)

    def line_up(p, b, act):
        @pl.when((b <= tensor) & (tensor < size_t - 1))
        def _():
            act(z_copy(b, p, above, b))

    def line_down(p, b, slot, act):
        @pl.when((b >= tensor) & (tensor > 0))
        def _():
            act(z_copy(b, p, below, slot))

    def start(copy):
        copy.start()

    def done(copy):
        copy.wait_send()

    sources = near_first()
    for p in range(PIECES):
        if line:
            line_up(p, tensor, start)
            line_down(p, tensor, size_t, start)
        else:
            for step, to, _ in others("tensor"):
                begin(z_copy(tensor, p, to, step - 1))
    pass_on(size_t - 1, tensor)
    on_block(section, tensor)
    from_sections(size_t - 1, tensor)

    def arrive(slot, p):
        source = sources[slot]
        z_copy(source, p, source, slot).wait_recv()
        if line:
            line_up(p, source, start)
            line_down(p, source, source, start)
        if p == PIECES - 1:
            pass_on(slot, source)

    for slot, source in enumerate(sources):
        for p in range(PIECES):
            arrive(slot, p)
            if slot > 0 and p == 0:
                on_block(section, sources[slot - 1])
        if slot > 0:
            from_sections(slot - 1, sources[slot - 1])
    last = len(sources) - 1
    on_block(section, sources[last])
    from_sections(last, sources[last])
    for copy in started:
        copy.wait_send()
    if line:
        for p in range(PIECES):
            line_down(p, tensor, size_t, done)
            for b in [tensor, *sources]:
                line_up(p, b, done)
            for b in sources:
                line_down(p, b, b, done)


def group_peers():
    return [{"tensor": to} for _, to, _ in others("tensor")] + [
        {"section": to} for _, to, _ in others("section")
    ]


def dma_sems(count):
    return pltpu.SemaphoreType.DMA((2, max(1, count)))


def near_first():
    tensor = lax.axis_index("tensor")
    if lax.axis_size("tensor") == 4:
        upper = tensor // 2
        return [tensor + 1 - 2 * lax.rem(tensor, 2), 2 - upper, 3 - 3 * upper]
    return [source for _, _, source in others("tensor")]


def block_order():
    section, tensor = lax.axis_index("section"), lax.axis_index("tensor")
    order = []
    for b in [tensor, *near_first()]:
        order += [(section, b)] + [(source, b) for _, _, source in others("section")]
    return order


def parts_of(block):
    return max(1, block // 16)


def times_gain(rows, gain32, first):
    tiles = range(rows.shape[1] // 128)
    return jnp.concatenate(
        [rows[:, i * 128 : (i + 1) * 128] * gain32[pl.ds(first + i, 1), :] for i in tiles], axis=1
    )


def front_body(
    x_ref, gain_ref, cos_ref, sin_ref, wq_hbm, wk_hbm, early, att_ref,
    gain32, blocks, wide, wk, qacc, kacc, stat, kv_src, kv_dst,
    sem_w, sem_own, sem_t, sem_s, sem_kv, sem_kv_out, after,
):
    section, tensor, me = lax.axis_index("section"), lax.axis_index("tensor"), lax.axis_index("dp")
    size_s, size_t, size_d = lax.axis_size("section"), lax.axis_size("tensor"), lax.axis_size("dp")
    count = size_s * size_t
    index = section * size_t + tensor
    local_rows, width = x_ref.shape
    features = count * width
    heads_dev = qacc.shape[1] // HD
    group_size = H // KVH
    units, _, unit = kv_src.shape
    pieces = HD // unit
    rep = group_size // heads_dev

    order = block_order()
    loads = []
    for k, (s, t) in enumerate(order):
        rows = pl.ds(pl.multiple_of((s * size_t + t) * width, width), width)
        loads.append(
            (
                pltpu.make_async_copy(wq_hbm.at[rows], wide.at[pl.ds(k * width, width)], sem_w.at[0, k]),
                pltpu.make_async_copy(wk_hbm.at[rows], wk.at[k], sem_w.at[1, k]),
            )
        )
    for pair in loads:
        for load in pair:
            load.start()
    own = pltpu.make_async_copy(x_ref, blocks.at[index], sem_own)
    own.start()
    gain32[...] = gain_ref[...].astype(F32)

    dps = others("dp")
    everyone = []
    for hop_s in range(size_s):
        for hop_t in range(size_t):
            for hop_d in range(size_d):
                if hop_s + hop_t + hop_d:
                    everyone.append(
                        {
                            "section": lax.rem(section + hop_s, size_s),
                            "tensor": lax.rem(tensor + hop_t, size_t),
                            "dp": lax.rem(me + hop_d, size_d),
                        }
                    )
    greet(everyone)
    own.wait()

    seen = []

    def on_block(s, t):
        k = len(seen)
        seen.append(k)
        for load in loads[k]:
            load.wait()
        early(k)
        at = s * size_t + t
        raw = blocks[at]
        rows = raw.astype(F32)
        part = jnp.sum(rows * rows, axis=-1, keepdims=True)
        stat[...] = part if k == 0 else stat[...] + part
        scaled = times_gain(rows, gain32, at * (width // 128)).astype(BF16)
        tile = tile_of(qacc.shape[1], GTILE)

        @pl.loop(0, qacc.shape[1] // tile)
        def _(j):
            cols = pl.ds(pl.multiple_of(j * tile, tile), tile)
            term = jnp.dot(scaled, wide[k * width : (k + 1) * width, cols], preferred_element_type=F32)
            qacc[:, cols] = term if k == 0 else qacc[:, cols] + term

        term = jnp.dot(scaled, wk[k], preferred_element_type=F32)
        kacc[...] = term if k == 0 else kacc[...] + term

    gather_group(blocks, sem_t, sem_s, on_block)
    for load in after:
        load.start()
    factor = lax.rsqrt(stat[...] * (1.0 / features) + EPS)

    for i in range(units):
        kv_src[i] = (kacc[:, i * unit : (i + 1) * unit] * factor).astype(BF16)

    def dp_rows(at):
        return pl.ds(pl.multiple_of(at * local_rows, local_rows), local_rows)

    half = KVH * pieces

    def kv_copy(i, r, g, kind, piece, step, to):
        return pltpu.make_async_remote_copy(
            src_ref=kv_src.at[i],
            dst_ref=kv_dst.at[kind, piece, dp_rows(me)],
            send_sem=sem_kv_out.at[(i * rep + r) * size_d + step],
            recv_sem=sem_kv.at[1, (kind * pieces + piece) * size_d + step],
            device_id={"section": g // size_t, "tensor": lax.rem(g, size_t), "dp": to},
            device_id_type=MESH,
        )

    hops = [(step, to, source) for step, to, source in dps] + [(0, me, me)]

    def each_send(act):
        for i in range(units):
            u = index * units + i
            kind, piece = u // half, lax.rem(u, pieces)
            head = lax.rem(u, half) // pieces
            for r in range(rep):
                g = head * rep + r
                for step, to, _ in hops:
                    if step:
                        act(kv_copy(i, r, g, kind, piece, step, to), i, kind, piece, False)
                    else:
                        @pl.when(g != index)
                        def _():
                            act(kv_copy(i, r, g, kind, piece, step, to), i, kind, piece, False)

                        @pl.when(g == index)
                        def _():
                            act(None, i, kind, piece, True)

    def begin(copy, i, kind, piece, local):
        if local:
            kv_dst[kind, piece, dp_rows(me), :] = kv_src[i]
        else:
            copy.start()

    each_send(begin)

    cosine, sine = cos_ref[dp_rows(me), :], sin_ref[dp_rows(me), :]
    queries = []
    for h in range(heads_dev):
        q = qacc[:, h * HD : (h + 1) * HD] * factor
        q = q * cosine + pltpu.roll(q, HD // 2, axis=1) * sine
        queries.append(q.astype(BF16))

    head = index // rep
    for kind in range(2):
        for piece in range(pieces):
            g = (kind * half + head * pieces + piece) // units
            for step, to, source in hops:
                dst = kv_dst.at[kind, piece, dp_rows(source)]
                wait = push(dst, dst, sem_kv, (kind * pieces + piece) * size_d + step, {"tensor": tensor})
                if step:
                    wait.wait_recv()
                else:
                    @pl.when(g != index)
                    def _():
                        wait.wait_recv()

    def whole(kind):
        return jnp.concatenate([kv_dst[kind, piece] for piece in range(pieces)], axis=1) if pieces > 1 else kv_dst[kind, 0]

    keys = whole(0).astype(F32)
    keys = (keys * cos_ref[...] + pltpu.roll(keys, HD // 2, axis=1) * sin_ref[...]).astype(BF16)
    values = whole(1)
    total_rows = keys.shape[0]
    block = total_rows // count
    parts = parts_of(block)
    sub = block // parts
    shape = (local_rows, total_rows)
    allowed = lax.broadcasted_iota(jnp.int32, shape, 1) <= (
        lax.broadcasted_iota(jnp.int32, shape, 0) + me * local_rows
    )
    for h in range(heads_dev):
        scores = lax.dot_general(
            queries[h], keys, (((1,), (1,)), ((), ())), preferred_element_type=F32
        ) * HD ** (-0.5)
        scores = jnp.where(allowed, scores, -1e30)
        expo = jnp.exp(scores - jnp.max(scores, axis=-1, keepdims=True))
        probs = (expo / jnp.sum(expo, axis=-1, keepdims=True)).astype(BF16)
        mixed = jnp.dot(probs, values, preferred_element_type=F32).astype(BF16)
        for k in range(parts):
            for j in range(local_rows // block):
                att_ref[k, j * sub : (j + 1) * sub, h * HD : (h + 1) * HD] = mixed[j * block + k * sub :][:sub]

    def end(copy, i, kind, piece, local):
        if not local:
            copy.wait_send()

    each_send(end)


def tile_of(width, most):
    return width if width <= most else most


def back_body(
    att_ref, blocks, gain_ref, loads, out_ref, gain32, wo, wide, wd, att_all, part, pair_rx, comb, z_rx, resid, stat_tx, stat_rx,
    nrm, scaled, gu, rx1, tx2, rx2, hid, part2, pair_rx2, comb2, z_rx2,
    sem_att, sem_res, sem_p, sem_z, sem_stat, sem_t, sem_s,
    sem_1, sem_2, sem_h, sem_p2, sem_z2,
):
    section, tensor, me = lax.axis_index("section"), lax.axis_index("tensor"), lax.axis_index("dp")
    size_t, size_d = lax.axis_size("tensor"), lax.axis_size("dp")
    group_index = section * size_t + tensor
    parts, dp_sub, width = att_ref.shape
    local_rows = parts * dp_sub
    count, _, span = blocks.shape
    features = count * span
    lumps, block, _ = resid.shape
    cols = lumps * span
    sub = block // parts
    chunks = gu.shape[1]
    dps, sections, tensors = others("dp"), others("section"), others("tensor")
    hops_s = len(sections)
    sends = []

    gain32[...] = gain_ref[...].astype(F32)

    def send(copy):
        copy.start()
        sends.append(copy)

    def dp_rows(index):
        return pl.ds(pl.multiple_of(index * dp_sub, dp_sub), dp_sub)

    def group_rows(s, t):
        return pl.ds(pl.multiple_of((s * size_t + t) * sub, sub), sub)

    def att_copy(k, step, to):
        return push(att_ref.at[k], att_all.at[k, dp_rows(me)], sem_att, k * (size_d - 1) + step - 1, {"dp": to})

    def att_start(k):
        for step, to, _ in dps:
            if k < parts:
                send(att_copy(k, step, to))

    att_start(0)
    per = local_rows // block
    holder = group_index // per
    held_rows = pl.ds(pl.multiple_of(lax.rem(group_index, per) * block, block), block)

    def resid_copy(step, to):
        src = blocks.at[pl.ds(to * lumps, lumps), held_rows]
        return push(src, resid, sem_res, step - 1, {"dp": to})

    loads[0].wait()
    att_start(1)

    @pl.when(me == holder)
    def _():
        for step, to, _ in dps:
            resid_copy(step, to).start()
        resid[...] = blocks[pl.ds(me * lumps, lumps), held_rows, :]

    for k in range(parts):
        att_all[k, dp_rows(me), :] = att_ref[k]
    tile = tile_of(cols, TILE)

    def pair_copy(k, source, rx, sem, hop, other, step, to):
        return push(
            source.at[k, group_rows(other, to)],
            rx.at[k, hop - 1, step],
            sem,
            (k * hops_s + hop - 1) * size_t + step,
            {"section": other},
        )

    def pair_start(k, source, rx, sem):
        for step, to in [(step, to) for step, to, _ in tensors] + [(0, tensor)]:
            for hop, other, _ in sections:
                send(pair_copy(k, source, rx, sem, hop, other, step, to))

    def paired(k, source, rx, sem, step, to):
        total = source[k, group_rows(section, to), :].astype(F32)
        for hop, other, _ in sections:
            pair_copy(k, source, rx, sem, hop, other, step, to).wait_recv()
            total = total + rx[k, hop - 1, step].astype(F32)
        return total

    def z_copy(k, out, rx, sem, step, to):
        return push(out.at[k, step - 1], rx.at[k, step - 1], sem, k * (size_t - 1) + step - 1, {"tensor": to})

    def z_start(k, source, rx, sem, out, z_in, sem_out):
        for step, to, _ in tensors:
            out[k, step - 1] = paired(k, source, rx, sem, step, to).astype(BF16)
            send(z_copy(k, out, z_in, sem_out, step, to))

    def z_total(k, source, rx, sem, out, z_in, sem_out):
        total = paired(k, source, rx, sem, 0, tensor)
        for step, to, _ in tensors:
            z_copy(k, out, z_in, sem_out, step, to).wait_recv()
            total = total + z_in[k, step - 1].astype(F32)
        return total

    first_set = (part, pair_rx, sem_p)
    last_set = (part2, pair_rx2, sem_p2)

    def head_out(k):
        for step, to, _ in dps:
            att_copy(k, step, to).wait_recv()
        att_start(k + 2)

        @pl.loop(0, cols // tile)
        def _(j):
            at = pl.ds(pl.multiple_of(j * tile, tile), tile)
            part[k, :, at] = jnp.dot(att_all[k], wo[:, at], preferred_element_type=F32).astype(BF16)

        pair_start(k, *first_set)

    def head_z(k):
        z_start(k, *first_set, comb, z_rx, sem_z)

    z_sends, z_arrivals = z_routes()

    def pass_copy(k, slot, b, to):
        at = nrm.at[k, group_rows(section, b)]
        return push(at, at, sem_t, k * (size_t - 1) + slot, {"tensor": to})

    def across(k, s, b, slot, hop, other):
        at = nrm.at[k, group_rows(s, b)]
        return push(at, at, sem_s, (k * size_t + slot) * hops_s + hop - 1, {"section": other})

    def share_block(k, b, slot):
        for hop, other, _ in sections:
            send(across(k, section, b, slot, hop, other))

    def middle(k):
        summed = z_total(k, *first_set, comb, z_rx, sem_z)
        if k == 0:
            for step, to, source in dps:
                @pl.when(source == holder)
                def _():
                    resid_copy(step, to).wait_recv()

        held = jnp.concatenate([resid[i, k * sub : (k + 1) * sub] for i in range(lumps)], axis=1)
        rows = (held.astype(F32) + summed).astype(BF16)
        nrm[k, group_rows(section, tensor), :] = rows
        for slot, to in z_sends:
            send(pass_copy(k, slot, tensor, to))
        share_block(k, tensor, size_t - 1)

    def relay(k):
        for slot, source, onward in z_arrivals:
            pass_copy(k, slot, source, source).wait_recv()
            if onward:
                send(pass_copy(k, onward[0], source, onward[1]))
            share_block(k, source, slot)

    def gathered(k):
        for slot, b in [(size_t - 1, tensor)] + [(slot, source) for slot, source, _ in z_arrivals]:
            for hop, other, source in sections:
                across(k, source, b, slot, hop, other).wait_recv()

    def stat_copy(k, step, to):
        return push(
            stat_tx.at[k, dp_rows(to)], stat_rx.at[k, step - 1], sem_stat, k * (size_d - 1) + step - 1, {"dp": to}
        )

    def scale(k):
        @pl.loop(0, stat_tx.shape[1] // 16)
        def _(j):
            at = pl.ds(pl.multiple_of(j * 16, 16), 16)
            rows = nrm[k, at, :].astype(F32)
            stat = jnp.sum(rows * rows, axis=-1, keepdims=True)
            stat_tx[k, at, :] = jnp.broadcast_to(stat, (16, 128))
            scaled[at, :] = times_gain(rows, gain32, me * (cols // 128)).astype(BF16)

        for step, to, _ in dps:
            send(stat_copy(k, step, to))

    factors = {}

    def factor_of(k):
        if k not in factors:
            stat = stat_tx[k, dp_rows(me), :][:, :1]
            for step, to, _ in dps:
                stat_copy(k, step, to).wait_recv()
                stat = stat + stat_rx[k, step - 1][:, :1]
            factors[k] = lax.rsqrt(stat * (1.0 / features) + EPS)
        return factors[k]

    share = gu.shape[3] // 2
    gtile = tile_of(share, GTILE)
    square = size_d == 4
    if square:
        x, y = lax.rem(me, 2), me // 2
        near = [y * 2 + (1 - x), (1 - y) * 2 + x]
        far_peer = (1 - y) * 2 + (1 - x)
    slots = 2 if square else size_d - 1
    hid_slots = size_d - 1

    def first_copy(k, c, slot, owner, to):
        return push(
            gu.at[k, c, dp_rows(owner)], rx1.at[k, c, slot], sem_1, (k * chunks + c) * slots + slot, {"dp": to}
        )

    def second_copy(k, c, to):
        return push(tx2.at[k, c], rx2.at[k, c], sem_2, k * chunks + c, {"dp": to})

    def hid_copy(k, c, owner, slot, to):
        at = hid.at[k, c, dp_rows(owner)]
        return push(at, at, sem_h, (k * chunks + c) * hid_slots + slot, {"dp": to})

    def gate_up(k):
        if k == 0:
            for load in loads[2:]:
                load.wait()
        scale(k)
        for c in range(chunks):
            @pl.loop(0, share // gtile)
            def _(j):
                lo = pl.ds(pl.multiple_of(j * gtile, gtile), gtile)
                hi = pl.ds(pl.multiple_of(share + j * gtile, gtile), gtile)
                for half, at in enumerate((lo, hi)):
                    first_row = (half * chunks + c) * cols
                    weights = wide[first_row : first_row + cols, lo]
                    gu[k, c, :, at] = jnp.dot(scaled[...], weights, preferred_element_type=F32).astype(BF16)

            if square:
                first = near[c % 2]
                send(first_copy(k, c, 1, far_peer, first))
                send(first_copy(k, c, 0, first, first))
            else:
                for step, to, _ in dps:
                    send(first_copy(k, c, step - 1, to, to))

    def second(k, c):
        if square:
            one, two = near[c % 2], near[1 - c % 2]
            first_copy(k, c, 1, far_peer, one).wait_recv()
            tx2[k, c] = (gu[k, c, dp_rows(two), :].astype(F32) + rx1[k, c, 1].astype(F32)).astype(BF16)
            send(second_copy(k, c, two))

    def hidden(k, c):
        both = gu[k, c, dp_rows(me), :].astype(F32)
        if square:
            one, two = near[c % 2], near[1 - c % 2]
            first_copy(k, c, 0, one, one).wait_recv()
            second_copy(k, c, two).wait_recv()
            both = both + rx1[k, c, 0].astype(F32) + rx2[k, c].astype(F32)
        else:
            for step, to, _ in dps:
                first_copy(k, c, step - 1, to, to).wait_recv()
                both = both + rx1[k, c, step - 1].astype(F32)
        both = both * factor_of(k)
        gate, upper = both[:, :share], both[:, share:]
        hid[k, c, dp_rows(me), :] = (gate / (1.0 + jnp.exp(-gate)) * upper).astype(BF16)
        targets = list(enumerate(near)) if square else [(step - 1, to) for step, to, _ in dps]
        for slot, to in targets:
            send(hid_copy(k, c, me, slot, to))

    def pass_hidden(k, c):
        if square:
            one, two = c % 2, 1 - c % 2
            hid_copy(k, c, near[one], one, near[one]).wait_recv()
            send(hid_copy(k, c, near[one], 2, near[two]))

    def down_wait(k, c):
        if k == 0 and c == 0:
            loads[1].wait()
        if square:
            two = 1 - c % 2
            arrivals = [(two, near[two]), (2, far_peer)]
        else:
            arrivals = [(step - 1, source) for step, _, source in dps]
        for slot, source in arrivals:
            hid_copy(k, c, source, slot, source).wait_recv()

    def down_out(k):
        @pl.loop(0, cols // tile)
        def _(j):
            at = pl.ds(pl.multiple_of(j * tile, tile), tile)
            term = jnp.dot(hid[k, 0], wd[:share, at], preferred_element_type=F32)
            for c in range(1, chunks):
                term = term + jnp.dot(hid[k, c], wd[c * share : (c + 1) * share, at], preferred_element_type=F32)
            part2[k, :, at] = term.astype(BF16)

        pair_start(k, *last_set)

    def down_z(k):
        z_start(k, *last_set, comb2, z_rx2, sem_z2)

    def finish(k):
        total = z_total(k, *last_set, comb2, z_rx2, sem_z2)
        out_ref[k * sub : (k + 1) * sub, :] = (nrm[k, group_rows(section, tensor), :].astype(F32) + total).astype(BF16)

    def each(act, k):
        return [(act, k, c) for c in range(chunks)]

    def add(act, k):
        if 0 <= k < parts and (act, k) not in added:
            added.append((act, k))
            plan.extend(each(act, k) if act in (second, hidden, pass_hidden, down_wait) else [(act, k)])

    added, plan = [], []
    names = {
        "H": head_out, "Z": head_z, "M": middle, "R": relay, "G": gathered, "U": gate_up, "S": second,
        "D": hidden, "P": pass_hidden, "V": down_wait, "W": down_out, "Y": down_z, "F": finish,
    }
    for line in ORDER:
        for step in line.split():
            add(names[step[0]], int(step[1]))
    for k in range(parts):
        for act in names.values():
            add(act, k)
    for act, *at in plan:
        act(*at)

    for copy in sends:
        copy.wait_send()
    @pl.when(me == holder)
    def _():
        for step, to, _ in dps:
            resid_copy(step, to).wait_send()


def body(
    x_ref, gain_a, gain_m, cos_ref, sin_ref, wq_hbm, wk_hbm, wo_hbm, wg_hbm, wu_hbm, wd_hbm, out_ref,
    att, blocks, wide, wk, wo, wd, sem_load, *rest,
):
    me = lax.axis_index("dp")
    cols, hidden_cols = wg_hbm.shape
    share = wide.shape[1]
    chunks = hidden_cols // share
    late = [
        pltpu.make_async_copy(wo_hbm.at[:, pl.ds(pl.multiple_of(me * cols, cols), cols)], wo, sem_load.at[0]),
        pltpu.make_async_copy(wd_hbm, wd, sem_load.at[1]),
    ]
    for half, source in enumerate((wg_hbm, wu_hbm)):
        for c in range(chunks):
            at = half * chunks + c
            late.append(
                pltpu.make_async_copy(
                    source.at[:, c * share : (c + 1) * share], wide.at[pl.ds(at * cols, cols)], sem_load.at[2 + at]
                )
            )

    def early(k):
        if k in (2, 4):
            late[k // 2 - 1].start()

    front_body(x_ref, gain_a, cos_ref, sin_ref, wq_hbm, wk_hbm, early, att, rest[0], blocks, wide, wk, *rest[1:12], late[2:])
    back_body(att, blocks, gain_m, late, out_ref, rest[0], wo, wide, wd, *rest[12:])


def layer(tokens, gain_a, gain_m, cosine, sine, w_query, w_keyval, w_out, w_gate, w_up, w_down, collective_id):
    size_s, size_t, size_d = lax.axis_size("section"), lax.axis_size("tensor"), lax.axis_size("dp")
    count = size_s * size_t
    local_rows, width = tokens.shape
    kv_cols = w_keyval.shape[1]
    unit = min(kv_cols, HD)
    pieces = HD // unit
    rep = (H // KVH) // (w_query.shape[1] // HD)
    arrivals = 2 * pieces * size_d
    block = local_rows * size_d // count
    parts = parts_of(block)
    dp_sub = local_rows // parts
    rows = dp_sub * size_d
    sub = block // parts
    heads_cols = w_query.shape[1]
    cols, wide = w_gate.shape
    share = heads_cols
    chunks = wide // share
    slots = 2 if size_d == 4 else size_d - 1
    scatter = [
        pltpu.VMEM((parts, rows, cols), BF16),
        pltpu.VMEM((parts, size_s - 1, size_t, sub, cols), BF16),
        pltpu.VMEM((parts, size_t - 1, sub, cols), BF16),
        pltpu.VMEM((parts, size_t - 1, sub, cols), BF16),
    ]
    return pl.pallas_call(
        body,
        out_shape=jax.ShapeDtypeStruct((parts * sub, cols), BF16),
        in_specs=[VMEM] * 5 + [ANY] * 6,
        out_specs=VMEM,
        scratch_shapes=[
            pltpu.VMEM((parts, dp_sub, heads_cols), BF16),
            pltpu.VMEM((count, local_rows, width), BF16),
            pltpu.VMEM((max(w_query.shape[0], 2 * chunks * cols), share), BF16),
            pltpu.VMEM((count, width, kv_cols), BF16),
            pltpu.VMEM((heads_cols, cols), BF16),
            pltpu.VMEM(w_down.shape, BF16),
            pltpu.SemaphoreType.DMA((2 + 2 * chunks,)),
            pltpu.VMEM(gain_a.shape, F32),
            pltpu.VMEM((local_rows, heads_cols), F32),
            pltpu.VMEM((local_rows, kv_cols), F32),
            pltpu.VMEM((local_rows, 1), F32),
            pltpu.VMEM((kv_cols // unit, local_rows, unit), BF16),
            pltpu.VMEM((2, pieces, local_rows * size_d, unit), BF16),
            pltpu.SemaphoreType.DMA((2, count)),
            pltpu.SemaphoreType.DMA,
            dma_sems((size_t + 1) * PIECES),
            dma_sems(size_t * (size_s - 1)),
            dma_sems(arrivals),
            pltpu.SemaphoreType.DMA((kv_cols // unit * rep * size_d,)),
            pltpu.VMEM((parts, rows, heads_cols), BF16),
            *scatter,
            pltpu.VMEM((cols // width, block, width), BF16),
            pltpu.VMEM((parts, rows, 128), F32),
            pltpu.VMEM((parts, size_d - 1, dp_sub, 128), F32),
            pltpu.VMEM((parts, rows, cols), BF16),
            pltpu.VMEM((rows, cols), BF16),
            pltpu.VMEM((parts, chunks, rows, 2 * share), BF16),
            pltpu.VMEM((parts, chunks, slots, dp_sub, 2 * share), BF16),
            pltpu.VMEM((parts, chunks, dp_sub, 2 * share), BF16),
            pltpu.VMEM((parts, chunks, dp_sub, 2 * share), BF16),
            pltpu.VMEM((parts, chunks, rows, share), BF16),
            *scatter,
            dma_sems(parts * (size_d - 1)),
            dma_sems(size_d - 1),
            dma_sems(parts * (size_s - 1) * size_t),
            dma_sems(parts * (size_t - 1)),
            dma_sems(parts * (size_d - 1)),
            dma_sems(parts * (size_t - 1)),
            dma_sems(parts * size_t * (size_s - 1)),
            dma_sems(parts * chunks * slots),
            dma_sems(parts * chunks),
            dma_sems(parts * chunks * (size_d - 1)),
            dma_sems(parts * (size_s - 1) * size_t),
            dma_sems(parts * (size_t - 1)),
        ],
        compiler_params=pltpu.CompilerParams(
            collective_id=collective_id, has_side_effects=True, vmem_limit_bytes=66000000
        ),
    )(tokens, gain_a, gain_m, cosine, sine, w_query, w_keyval, w_out, w_gate, w_up, w_down)


def shards(tokens_in, gain_attn, w_query, w_keyval, w_out, gain_mlp, w_gate, w_up, w_down):
    local_rows, width = tokens_in.shape
    total_rows = local_rows * lax.axis_size("dp")
    frequency = THETA ** (-np.arange(HD // 2) * 2.0 / HD)
    angles = np.arange(total_rows)[:, None] * frequency[None, :]
    cosine, sine = np.cos(angles), np.sin(angles)
    return layer(
        tokens_in,
        gain_attn.reshape(-1, 128),
        gain_mlp.reshape(-1, 128),
        jnp.asarray(np.concatenate([cosine, cosine], axis=1), F32),
        jnp.asarray(np.concatenate([-sine, sine], axis=1), F32),
        w_query,
        w_keyval,
        w_out,
        w_gate,
        w_up,
        w_down,
        1,
    )


def solution(mesh):
    placed = (
        P("dp", ("section", "tensor")),
        P(),
        P(None, ("section", "tensor")),
        P(None, ("section", "tensor")),
        P(("section", "tensor"), None),
        P(),
        P("dp", ("section", "tensor")),
        P("dp", ("section", "tensor")),
        P(("section", "tensor"), "dp"),
    )
    return jax.shard_map(
        shards,
        mesh=mesh,
        in_specs=placed,
        out_specs=P(("section", "tensor"), "dp"),
        check_vma=False,
    )
```

```python
import jax
import jax.numpy as jnp
import numpy as np
from jax import lax
from jax.experimental import pallas as pl
from jax.experimental.pallas import tpu as pltpu
from jax.sharding import PartitionSpec as P

H = 64
KVH = 8
HD = 128
EPS = 1e-05
THETA = 10000.0
TILE = 1024
GTILE = 1024
PIECES = 4
ORDER = (
    "H0 Z0 H1 Z1",
    "M0 H2 M1 R0",
    "G0 Z2 U0 H3",
    "R1 G1 Z3 U1",
    "S0 M2 S1 D0",
    "M3 R2 P0 G2",
    "D1 U2 R3 G3",
    "U3 S2 P1 V0",
    "W0 S3 Y0 D2",
    "D3 P2 V1 W1",
    "Y1 P3 F0 V2",
    "W2 Y2 V3 W3",
    "Y3 F1 F2 F3",
)
MESH = pl.DeviceIdType.MESH
F32 = jnp.float32
BF16 = jnp.bfloat16
VMEM = pl.BlockSpec(memory_space=pltpu.VMEM)
ANY = pl.BlockSpec(memory_space=pl.ANY)


def greet(peers):
    barrier = pltpu.get_barrier_semaphore()
    for peer in peers:
        pl.semaphore_signal(barrier, inc=1, device_id=peer, device_id_type=MESH)
    pl.semaphore_wait(barrier, len(peers))


def push(src, dst, sems, slot, device):
    return pltpu.make_async_remote_copy(
        src_ref=src,
        dst_ref=dst,
        send_sem=sems.at[0, slot],
        recv_sem=sems.at[1, slot],
        device_id=device,
        device_id_type=MESH,
    )


def others(axis):
    size = lax.axis_size(axis)
    me = lax.axis_index(axis)
    return [(step, lax.rem(me + step, size), lax.rem(me + size - step, size)) for step in range(1, size)]


def z_routes():
    hops = others("tensor")
    return [(step - 1, to) for step, to, _ in hops], [(step - 1, source, None) for step, _, source in hops]


def gather_group(out, sem_t, sem_s, on_block):
    section, tensor = lax.axis_index("section"), lax.axis_index("tensor")
    sections = others("section")
    size_t = lax.axis_size("tensor")
    piece = out.shape[1] // PIECES
    line = size_t == 4
    started = []

    def begin(copy):
        copy.start()
        started.append(copy)

    def z_copy(b, p, to, slot):
        rows = out.at[section * size_t + b, pl.ds(p * piece, piece)]
        return pltpu.make_async_remote_copy(
            src_ref=rows,
            dst_ref=rows,
            send_sem=sem_t.at[0, slot * PIECES + p],
            recv_sem=sem_t.at[1, (b if line else slot) * PIECES + p],
            device_id={"tensor": to},
            device_id_type=MESH,
        )

    def s_copy(slot, s, b, step, to):
        block = out.at[s * size_t + b]
        return push(block, block, sem_s, slot * len(sections) + step - 1, {"section": to})

    def pass_on(slot, b):
        for step, to, _ in sections:
            begin(s_copy(slot, section, b, step, to))

    def from_sections(slot, b):
        for step, to, source in sections:
            s_copy(slot, source, b, step, to).wait_recv()
            on_block(source, b)

    above, below = lax.rem(tensor + 1, size_t), lax.rem(tensor + size_t - 1, size_t)

    def line_up(p, b, act):
        @pl.when((b <= tensor) & (tensor < size_t - 1))
        def _():
            act(z_copy(b, p, above, b))

    def line_down(p, b, slot, act):
        @pl.when((b >= tensor) & (tensor > 0))
        def _():
            act(z_copy(b, p, below, slot))

    def start(copy):
        copy.start()

    def done(copy):
        copy.wait_send()

    sources = near_first()
    for p in range(PIECES):
        if line:
            line_up(p, tensor, start)
            line_down(p, tensor, size_t, start)
        else:
            for step, to, _ in others("tensor"):
                begin(z_copy(tensor, p, to, step - 1))
    pass_on(size_t - 1, tensor)
    on_block(section, tensor)
    from_sections(size_t - 1, tensor)

    def arrive(slot, p):
        source = sources[slot]
        z_copy(source, p, source, slot).wait_recv()
        if line:
            line_up(p, source, start)
            line_down(p, source, source, start)
        if p == PIECES - 1:
            pass_on(slot, source)

    for slot, source in enumerate(sources):
        for p in range(PIECES):
            arrive(slot, p)
            if slot > 0 and p == 0:
                on_block(section, sources[slot - 1])
        if slot > 0:
            from_sections(slot - 1, sources[slot - 1])
    last = len(sources) - 1
    on_block(section, sources[last])
    from_sections(last, sources[last])
    for copy in started:
        copy.wait_send()
    if line:
        for p in range(PIECES):
            line_down(p, tensor, size_t, done)
            for b in [tensor, *sources]:
                line_up(p, b, done)
            for b in sources:
                line_down(p, b, b, done)


def group_peers():
    return [{"tensor": to} for _, to, _ in others("tensor")] + [
        {"section": to} for _, to, _ in others("section")
    ]


def dma_sems(count):
    return pltpu.SemaphoreType.DMA((2, max(1, count)))


def near_first():
    tensor = lax.axis_index("tensor")
    if lax.axis_size("tensor") == 4:
        upper = tensor // 2
        return [tensor + 1 - 2 * lax.rem(tensor, 2), 2 - upper, 3 - 3 * upper]
    return [source for _, _, source in others("tensor")]


def block_order():
    section, tensor = lax.axis_index("section"), lax.axis_index("tensor")
    order = []
    for b in [tensor, *near_first()]:
        order += [(section, b)] + [(source, b) for _, _, source in others("section")]
    return order


def parts_of(block):
    return max(1, block // 16)


def times_gain(rows, gain32, first):
    tiles = range(rows.shape[1] // 128)
    return jnp.concatenate(
        [rows[:, i * 128 : (i + 1) * 128] * gain32[pl.ds(first + i, 1), :] for i in tiles], axis=1
    )


def front_body(
    x_ref, gain_ref, cos_ref, sin_ref, wq_hbm, wk_hbm, early, att_ref,
    gain32, blocks, wide, wk, qacc, kacc, stat, kv_src, kv_dst,
    sem_w, sem_own, sem_t, sem_s, sem_kv, sem_kv_out, after,
):
    section, tensor, me = lax.axis_index("section"), lax.axis_index("tensor"), lax.axis_index("dp")
    size_s, size_t, size_d = lax.axis_size("section"), lax.axis_size("tensor"), lax.axis_size("dp")
    count = size_s * size_t
    index = section * size_t + tensor
    local_rows, width = x_ref.shape
    features = count * width
    heads_dev = qacc.shape[1] // HD
    group_size = H // KVH
    units, _, unit = kv_src.shape
    pieces = HD // unit
    rep = group_size // heads_dev

    order = block_order()
    loads = []
    for k, (s, t) in enumerate(order):
        rows = pl.ds(pl.multiple_of((s * size_t + t) * width, width), width)
        loads.append(
            (
                pltpu.make_async_copy(wq_hbm.at[rows], wide.at[pl.ds(k * width, width)], sem_w.at[0, k]),
                pltpu.make_async_copy(wk_hbm.at[rows], wk.at[k], sem_w.at[1, k]),
            )
        )
    for pair in loads:
        for load in pair:
            load.start()
    own = pltpu.make_async_copy(x_ref, blocks.at[index], sem_own)
    own.start()
    gain32[...] = gain_ref[...].astype(F32)

    dps = others("dp")
    everyone = []
    for hop_s in range(size_s):
        for hop_t in range(size_t):
            for hop_d in range(size_d):
                if hop_s + hop_t + hop_d:
                    everyone.append(
                        {
                            "section": lax.rem(section + hop_s, size_s),
                            "tensor": lax.rem(tensor + hop_t, size_t),
                            "dp": lax.rem(me + hop_d, size_d),
                        }
                    )
    greet(everyone)
    own.wait()

    seen = []

    def on_block(s, t):
        k = len(seen)
        seen.append(k)
        for load in loads[k]:
            load.wait()
        early(k)
        at = s * size_t + t
        raw = blocks[at]
        rows = raw.astype(F32)
        part = jnp.sum(rows * rows, axis=-1, keepdims=True)
        stat[...] = part if k == 0 else stat[...] + part
        scaled = times_gain(rows, gain32, at * (width // 128)).astype(BF16)
        tile = tile_of(qacc.shape[1], GTILE)

        @pl.loop(0, qacc.shape[1] // tile)
        def _(j):
            cols = pl.ds(pl.multiple_of(j * tile, tile), tile)
            term = jnp.dot(scaled, wide[k * width : (k + 1) * width, cols], preferred_element_type=F32)
            qacc[:, cols] = term if k == 0 else qacc[:, cols] + term

        term = jnp.dot(scaled, wk[k], preferred_element_type=F32)
        kacc[...] = term if k == 0 else kacc[...] + term

    gather_group(blocks, sem_t, sem_s, on_block)
    for load in after:
        load.start()
    factor = lax.rsqrt(stat[...] * (1.0 / features) + EPS)

    for i in range(units):
        kv_src[i] = (kacc[:, i * unit : (i + 1) * unit] * factor).astype(BF16)

    def dp_rows(at):
        return pl.ds(pl.multiple_of(at * local_rows, local_rows), local_rows)

    half = KVH * pieces

    def kv_copy(i, r, g, kind, piece, step, to):
        return pltpu.make_async_remote_copy(
            src_ref=kv_src.at[i],
            dst_ref=kv_dst.at[kind, piece, dp_rows(me)],
            send_sem=sem_kv_out.at[(i * rep + r) * size_d + step],
            recv_sem=sem_kv.at[1, (kind * pieces + piece) * size_d + step],
            device_id={"section": g // size_t, "tensor": lax.rem(g, size_t), "dp": to},
            device_id_type=MESH,
        )

    hops = [(step, to, source) for step, to, source in dps] + [(0, me, me)]

    def each_send(act):
        for i in range(units):
            u = index * units + i
            kind, piece = u // half, lax.rem(u, pieces)
            head = lax.rem(u, half) // pieces
            for r in range(rep):
                g = head * rep + r
                for step, to, _ in hops:
                    if step:
                        act(kv_copy(i, r, g, kind, piece, step, to), i, kind, piece, False)
                    else:
                        @pl.when(g != index)
                        def _():
                            act(kv_copy(i, r, g, kind, piece, step, to), i, kind, piece, False)

                        @pl.when(g == index)
                        def _():
                            act(None, i, kind, piece, True)

    def begin(copy, i, kind, piece, local):
        if local:
            kv_dst[kind, piece, dp_rows(me), :] = kv_src[i]
        else:
            copy.start()

    each_send(begin)

    cosine, sine = cos_ref[dp_rows(me), :], sin_ref[dp_rows(me), :]
    queries = []
    for h in range(heads_dev):
        q = qacc[:, h * HD : (h + 1) * HD] * factor
        q = q * cosine + pltpu.roll(q, HD // 2, axis=1) * sine
        queries.append(q.astype(BF16))

    head = index // rep
    for kind in range(2):
        for piece in range(pieces):
            g = (kind * half + head * pieces + piece) // units
            for step, to, source in hops:
                dst = kv_dst.at[kind, piece, dp_rows(source)]
                wait = push(dst, dst, sem_kv, (kind * pieces + piece) * size_d + step, {"tensor": tensor})
                if step:
                    wait.wait_recv()
                else:
                    @pl.when(g != index)
                    def _():
                        wait.wait_recv()

    def whole(kind):
        return jnp.concatenate([kv_dst[kind, piece] for piece in range(pieces)], axis=1) if pieces > 1 else kv_dst[kind, 0]

    keys = whole(0).astype(F32)
    keys = (keys * cos_ref[...] + pltpu.roll(keys, HD // 2, axis=1) * sin_ref[...]).astype(BF16)
    values = whole(1)
    total_rows = keys.shape[0]
    block = total_rows // count
    parts = parts_of(block)
    sub = block // parts
    shape = (local_rows, total_rows)
    allowed = lax.broadcasted_iota(jnp.int32, shape, 1) <= (
        lax.broadcasted_iota(jnp.int32, shape, 0) + me * local_rows
    )
    for h in range(heads_dev):
        scores = lax.dot_general(
            queries[h], keys, (((1,), (1,)), ((), ())), preferred_element_type=F32
        ) * HD ** (-0.5)
        scores = jnp.where(allowed, scores, -1e30)
        expo = jnp.exp(scores - jnp.max(scores, axis=-1, keepdims=True))
        probs = (expo / jnp.sum(expo, axis=-1, keepdims=True)).astype(BF16)
        mixed = jnp.dot(probs, values, preferred_element_type=F32).astype(BF16)
        for k in range(parts):
            for j in range(local_rows // block):
                att_ref[k, j * sub : (j + 1) * sub, h * HD : (h + 1) * HD] = mixed[j * block + k * sub :][:sub]

    def end(copy, i, kind, piece, local):
        if not local:
            copy.wait_send()

    each_send(end)


def tile_of(width, most):
    return width if width <= most else most


def back_body(
    att_ref, blocks, gain_ref, loads, out_ref, gain32, wo, wide, wd, att_all, part, pair_rx, comb, z_rx, resid, stat_tx, stat_rx,
    nrm, scaled, gu, rx1, tx2, rx2, hid, part2, pair_rx2, comb2, z_rx2,
    sem_att, sem_res, sem_p, sem_z, sem_stat, sem_t, sem_s,
    sem_1, sem_2, sem_h, sem_p2, sem_z2,
):
    section, tensor, me = lax.axis_index("section"), lax.axis_index("tensor"), lax.axis_index("dp")
    size_t, size_d = lax.axis_size("tensor"), lax.axis_size("dp")
    group_index = section * size_t + tensor
    parts, dp_sub, width = att_ref.shape
    local_rows = parts * dp_sub
    count, _, span = blocks.shape
    features = count * span
    lumps, block, _ = resid.shape
    cols = lumps * span
    sub = block // parts
    chunks = gu.shape[1]
    dps, sections, tensors = others("dp"), others("section"), others("tensor")
    hops_s = len(sections)
    sends = []

    gain32[...] = gain_ref[...].astype(F32)

    def send(copy):
        copy.start()
        sends.append(copy)

    def dp_rows(index):
        return pl.ds(pl.multiple_of(index * dp_sub, dp_sub), dp_sub)

    def group_rows(s, t):
        return pl.ds(pl.multiple_of((s * size_t + t) * sub, sub), sub)

    def att_copy(k, step, to):
        return push(att_ref.at[k], att_all.at[k, dp_rows(me)], sem_att, k * (size_d - 1) + step - 1, {"dp": to})

    def att_start(k):
        for step, to, _ in dps:
            if k < parts:
                send(att_copy(k, step, to))

    att_start(0)
    per = local_rows // block
    holder = group_index // per
    held_rows = pl.ds(pl.multiple_of(lax.rem(group_index, per) * block, block), block)

    def resid_copy(step, to):
        src = blocks.at[pl.ds(to * lumps, lumps), held_rows]
        return push(src, resid, sem_res, step - 1, {"dp": to})

    loads[0].wait()
    att_start(1)

    @pl.when(me == holder)
    def _():
        for step, to, _ in dps:
            resid_copy(step, to).start()
        resid[...] = blocks[pl.ds(me * lumps, lumps), held_rows, :]

    for k in range(parts):
        att_all[k, dp_rows(me), :] = att_ref[k]
    tile = tile_of(cols, TILE)

    def pair_copy(k, source, rx, sem, hop, other, step, to):
        return push(
            source.at[k, group_rows(other, to)],
            rx.at[k, hop - 1, step],
            sem,
            (k * hops_s + hop - 1) * size_t + step,
            {"section": other},
        )

    def pair_start(k, source, rx, sem):
        for step, to in [(step, to) for step, to, _ in tensors] + [(0, tensor)]:
            for hop, other, _ in sections:
                send(pair_copy(k, source, rx, sem, hop, other, step, to))

    def paired(k, source, rx, sem, step, to):
        total = source[k, group_rows(section, to), :].astype(F32)
        for hop, other, _ in sections:
            pair_copy(k, source, rx, sem, hop, other, step, to).wait_recv()
            total = total + rx[k, hop - 1, step].astype(F32)
        return total

    def z_copy(k, out, rx, sem, step, to):
        return push(out.at[k, step - 1], rx.at[k, step - 1], sem, k * (size_t - 1) + step - 1, {"tensor": to})

    def z_start(k, source, rx, sem, out, z_in, sem_out):
        for step, to, _ in tensors:
            out[k, step - 1] = paired(k, source, rx, sem, step, to).astype(BF16)
            send(z_copy(k, out, z_in, sem_out, step, to))

    def z_total(k, source, rx, sem, out, z_in, sem_out):
        total = paired(k, source, rx, sem, 0, tensor)
        for step, to, _ in tensors:
            z_copy(k, out, z_in, sem_out, step, to).wait_recv()
            total = total + z_in[k, step - 1].astype(F32)
        return total

    first_set = (part, pair_rx, sem_p)
    last_set = (part2, pair_rx2, sem_p2)

    def head_out(k):
        for step, to, _ in dps:
            att_copy(k, step, to).wait_recv()
        att_start(k + 2)

        @pl.loop(0, cols // tile)
        def _(j):
            at = pl.ds(pl.multiple_of(j * tile, tile), tile)
            part[k, :, at] = jnp.dot(att_all[k], wo[:, at], preferred_element_type=F32).astype(BF16)

        pair_start(k, *first_set)

    def head_z(k):
        z_start(k, *first_set, comb, z_rx, sem_z)

    z_sends, z_arrivals = z_routes()

    def pass_copy(k, slot, b, to):
        at = nrm.at[k, group_rows(section, b)]
        return push(at, at, sem_t, k * (size_t - 1) + slot, {"tensor": to})

    def across(k, s, b, slot, hop, other):
        at = nrm.at[k, group_rows(s, b)]
        return push(at, at, sem_s, (k * size_t + slot) * hops_s + hop - 1, {"section": other})

    def share_block(k, b, slot):
        for hop, other, _ in sections:
            send(across(k, section, b, slot, hop, other))

    def middle(k):
        summed = z_total(k, *first_set, comb, z_rx, sem_z)
        if k == 0:
            for step, to, source in dps:
                @pl.when(source == holder)
                def _():
                    resid_copy(step, to).wait_recv()

        held = jnp.concatenate([resid[i, k * sub : (k + 1) * sub] for i in range(lumps)], axis=1)
        rows = (held.astype(F32) + summed).astype(BF16)
        nrm[k, group_rows(section, tensor), :] = rows
        for slot, to in z_sends:
            send(pass_copy(k, slot, tensor, to))
        share_block(k, tensor, size_t - 1)

    def relay(k):
        for slot, source, onward in z_arrivals:
            pass_copy(k, slot, source, source).wait_recv()
            if onward:
                send(pass_copy(k, onward[0], source, onward[1]))
            share_block(k, source, slot)

    def gathered(k):
        for slot, b in [(size_t - 1, tensor)] + [(slot, source) for slot, source, _ in z_arrivals]:
            for hop, other, source in sections:
                across(k, source, b, slot, hop, other).wait_recv()

    def stat_copy(k, step, to):
        return push(
            stat_tx.at[k, dp_rows(to)], stat_rx.at[k, step - 1], sem_stat, k * (size_d - 1) + step - 1, {"dp": to}
        )

    def scale(k):
        @pl.loop(0, stat_tx.shape[1] // 16)
        def _(j):
            at = pl.ds(pl.multiple_of(j * 16, 16), 16)
            rows = nrm[k, at, :].astype(F32)
            stat = jnp.sum(rows * rows, axis=-1, keepdims=True)
            stat_tx[k, at, :] = jnp.broadcast_to(stat, (16, 128))
            scaled[at, :] = times_gain(rows, gain32, me * (cols // 128)).astype(BF16)

        for step, to, _ in dps:
            send(stat_copy(k, step, to))

    factors = {}

    def factor_of(k):
        if k not in factors:
            stat = stat_tx[k, dp_rows(me), :][:, :1]
            for step, to, _ in dps:
                stat_copy(k, step, to).wait_recv()
                stat = stat + stat_rx[k, step - 1][:, :1]
            factors[k] = lax.rsqrt(stat * (1.0 / features) + EPS)
        return factors[k]

    share = gu.shape[3] // 2
    gtile = tile_of(share, GTILE)
    square = size_d == 4
    if square:
        x, y = lax.rem(me, 2), me // 2
        near = [y * 2 + (1 - x), (1 - y) * 2 + x]
        far_peer = (1 - y) * 2 + (1 - x)
    slots = 2 if square else size_d - 1
    hid_slots = size_d - 1

    def first_copy(k, c, slot, owner, to):
        return push(
            gu.at[k, c, dp_rows(owner)], rx1.at[k, c, slot], sem_1, (k * chunks + c) * slots + slot, {"dp": to}
        )

    def second_copy(k, c, to):
        return push(tx2.at[k, c], rx2.at[k, c], sem_2, k * chunks + c, {"dp": to})

    def hid_copy(k, c, owner, slot, to):
        at = hid.at[k, c, dp_rows(owner)]
        return push(at, at, sem_h, (k * chunks + c) * hid_slots + slot, {"dp": to})

    def gate_up(k):
        if k == 0:
            for load in loads[2:]:
                load.wait()
        scale(k)
        for c in range(chunks):
            @pl.loop(0, share // gtile)
            def _(j):
                lo = pl.ds(pl.multiple_of(j * gtile, gtile), gtile)
                hi = pl.ds(pl.multiple_of(share + j * gtile, gtile), gtile)
                for half, at in enumerate((lo, hi)):
                    first_row = (half * chunks + c) * cols
                    weights = wide[first_row : first_row + cols, lo]
                    gu[k, c, :, at] = jnp.dot(scaled[...], weights, preferred_element_type=F32).astype(BF16)

            if square:
                first = near[c % 2]
                send(first_copy(k, c, 1, far_peer, first))
                send(first_copy(k, c, 0, first, first))
            else:
                for step, to, _ in dps:
                    send(first_copy(k, c, step - 1, to, to))

    def second(k, c):
        if square:
            one, two = near[c % 2], near[1 - c % 2]
            first_copy(k, c, 1, far_peer, one).wait_recv()
            tx2[k, c] = (gu[k, c, dp_rows(two), :].astype(F32) + rx1[k, c, 1].astype(F32)).astype(BF16)
            send(second_copy(k, c, two))

    def hidden(k, c):
        both = gu[k, c, dp_rows(me), :].astype(F32)
        if square:
            one, two = near[c % 2], near[1 - c % 2]
            first_copy(k, c, 0, one, one).wait_recv()
            second_copy(k, c, two).wait_recv()
            both = both + rx1[k, c, 0].astype(F32) + rx2[k, c].astype(F32)
        else:
            for step, to, _ in dps:
                first_copy(k, c, step - 1, to, to).wait_recv()
                both = both + rx1[k, c, step - 1].astype(F32)
        both = both * factor_of(k)
        gate, upper = both[:, :share], both[:, share:]
        hid[k, c, dp_rows(me), :] = (gate / (1.0 + jnp.exp(-gate)) * upper).astype(BF16)
        targets = list(enumerate(near)) if square else [(step - 1, to) for step, to, _ in dps]
        for slot, to in targets:
            send(hid_copy(k, c, me, slot, to))

    def pass_hidden(k, c):
        if square:
            one, two = c % 2, 1 - c % 2
            hid_copy(k, c, near[one], one, near[one]).wait_recv()
            send(hid_copy(k, c, near[one], 2, near[two]))

    def down_wait(k, c):
        if k == 0 and c == 0:
            loads[1].wait()
        if square:
            two = 1 - c % 2
            arrivals = [(two, near[two]), (2, far_peer)]
        else:
            arrivals = [(step - 1, source) for step, _, source in dps]
        for slot, source in arrivals:
            hid_copy(k, c, source, slot, source).wait_recv()

    def down_out(k):
        @pl.loop(0, cols // tile)
        def _(j):
            at = pl.ds(pl.multiple_of(j * tile, tile), tile)
            term = jnp.dot(hid[k, 0], wd[:share, at], preferred_element_type=F32)
            for c in range(1, chunks):
                term = term + jnp.dot(hid[k, c], wd[c * share : (c + 1) * share, at], preferred_element_type=F32)
            part2[k, :, at] = term.astype(BF16)

        pair_start(k, *last_set)

    def down_z(k):
        z_start(k, *last_set, comb2, z_rx2, sem_z2)

    def finish(k):
        total = z_total(k, *last_set, comb2, z_rx2, sem_z2)
        out_ref[k * sub : (k + 1) * sub, :] = (nrm[k, group_rows(section, tensor), :].astype(F32) + total).astype(BF16)

    def each(act, k):
        return [(act, k, c) for c in range(chunks)]

    def add(act, k):
        if 0 <= k < parts and (act, k) not in added:
            added.append((act, k))
            plan.extend(each(act, k) if act in (second, hidden, pass_hidden, down_wait) else [(act, k)])

    added, plan = [], []
    names = {
        "H": head_out, "Z": head_z, "M": middle, "R": relay, "G": gathered, "U": gate_up, "S": second,
        "D": hidden, "P": pass_hidden, "V": down_wait, "W": down_out, "Y": down_z, "F": finish,
    }
    for line in ORDER:
        for step in line.split():
            add(names[step[0]], int(step[1]))
    for k in range(parts):
        for act in names.values():
            add(act, k)
    for act, *at in plan:
        act(*at)

    for copy in sends:
        copy.wait_send()
    @pl.when(me == holder)
    def _():
        for step, to, _ in dps:
            resid_copy(step, to).wait_send()


def body(
    x_ref, gain_a, gain_m, cos_ref, sin_ref, wq_hbm, wk_hbm, wo_hbm, wg_hbm, wu_hbm, wd_hbm, out_ref,
    att, blocks, wide, wk, wo, wd, sem_load, *rest,
):
    me = lax.axis_index("dp")
    cols, hidden_cols = wg_hbm.shape
    share = wide.shape[1]
    chunks = hidden_cols // share
    late = [
        pltpu.make_async_copy(wo_hbm.at[:, pl.ds(pl.multiple_of(me * cols, cols), cols)], wo, sem_load.at[0]),
        pltpu.make_async_copy(wd_hbm, wd, sem_load.at[1]),
    ]
    for half, source in enumerate((wg_hbm, wu_hbm)):
        for c in range(chunks):
            at = half * chunks + c
            late.append(
                pltpu.make_async_copy(
                    source.at[:, c * share : (c + 1) * share], wide.at[pl.ds(at * cols, cols)], sem_load.at[2 + at]
                )
            )

    def early(k):
        if k in (2, 4):
            late[k // 2 - 1].start()

    front_body(x_ref, gain_a, cos_ref, sin_ref, wq_hbm, wk_hbm, early, att, rest[0], blocks, wide, wk, *rest[1:12], late[2:])
    back_body(att, blocks, gain_m, late, out_ref, rest[0], wo, wide, wd, *rest[12:])


def layer(tokens, gain_a, gain_m, cosine, sine, w_query, w_keyval, w_out, w_gate, w_up, w_down, collective_id):
    size_s, size_t, size_d = lax.axis_size("section"), lax.axis_size("tensor"), lax.axis_size("dp")
    count = size_s * size_t
    local_rows, width = tokens.shape
    kv_cols = w_keyval.shape[1]
    unit = min(kv_cols, HD)
    pieces = HD // unit
    rep = (H // KVH) // (w_query.shape[1] // HD)
    arrivals = 2 * pieces * size_d
    block = local_rows * size_d // count
    parts = parts_of(block)
    dp_sub = local_rows // parts
    rows = dp_sub * size_d
    sub = block // parts
    heads_cols = w_query.shape[1]
    cols, wide = w_gate.shape
    share = heads_cols
    chunks = wide // share
    slots = 2 if size_d == 4 else size_d - 1
    scatter = [
        pltpu.VMEM((parts, rows, cols), BF16),
        pltpu.VMEM((parts, size_s - 1, size_t, sub, cols), BF16),
        pltpu.VMEM((parts, size_t - 1, sub, cols), BF16),
        pltpu.VMEM((parts, size_t - 1, sub, cols), BF16),
    ]
    return pl.pallas_call(
        body,
        out_shape=jax.ShapeDtypeStruct((parts * sub, cols), BF16),
        in_specs=[VMEM] * 5 + [ANY] * 6,
        out_specs=VMEM,
        scratch_shapes=[
            pltpu.VMEM((parts, dp_sub, heads_cols), BF16),
            pltpu.VMEM((count, local_rows, width), BF16),
            pltpu.VMEM((max(w_query.shape[0], 2 * chunks * cols), share), BF16),
            pltpu.VMEM((count, width, kv_cols), BF16),
            pltpu.VMEM((heads_cols, cols), BF16),
            pltpu.VMEM(w_down.shape, BF16),
            pltpu.SemaphoreType.DMA((2 + 2 * chunks,)),
            pltpu.VMEM(gain_a.shape, F32),
            pltpu.VMEM((local_rows, heads_cols), F32),
            pltpu.VMEM((local_rows, kv_cols), F32),
            pltpu.VMEM((local_rows, 1), F32),
            pltpu.VMEM((kv_cols // unit, local_rows, unit), BF16),
            pltpu.VMEM((2, pieces, local_rows * size_d, unit), BF16),
            pltpu.SemaphoreType.DMA((2, count)),
            pltpu.SemaphoreType.DMA,
            dma_sems((size_t + 1) * PIECES),
            dma_sems(size_t * (size_s - 1)),
            dma_sems(arrivals),
            pltpu.SemaphoreType.DMA((kv_cols // unit * rep * size_d,)),
            pltpu.VMEM((parts, rows, heads_cols), BF16),
            *scatter,
            pltpu.VMEM((cols // width, block, width), BF16),
            pltpu.VMEM((parts, rows, 128), F32),
            pltpu.VMEM((parts, size_d - 1, dp_sub, 128), F32),
            pltpu.VMEM((parts, rows, cols), BF16),
            pltpu.VMEM((rows, cols), BF16),
            pltpu.VMEM((parts, chunks, rows, 2 * share), BF16),
            pltpu.VMEM((parts, chunks, slots, dp_sub, 2 * share), BF16),
            pltpu.VMEM((parts, chunks, dp_sub, 2 * share), BF16),
            pltpu.VMEM((parts, chunks, dp_sub, 2 * share), BF16),
            pltpu.VMEM((parts, chunks, rows, share), BF16),
            *scatter,
            dma_sems(parts * (size_d - 1)),
            dma_sems(size_d - 1),
            dma_sems(parts * (size_s - 1) * size_t),
            dma_sems(parts * (size_t - 1)),
            dma_sems(parts * (size_d - 1)),
            dma_sems(parts * (size_t - 1)),
            dma_sems(parts * size_t * (size_s - 1)),
            dma_sems(parts * chunks * slots),
            dma_sems(parts * chunks),
            dma_sems(parts * chunks * (size_d - 1)),
            dma_sems(parts * (size_s - 1) * size_t),
            dma_sems(parts * (size_t - 1)),
        ],
        compiler_params=pltpu.CompilerParams(
            collective_id=collective_id, has_side_effects=True, vmem_limit_bytes=66000000
        ),
    )(tokens, gain_a, gain_m, cosine, sine, w_query, w_keyval, w_out, w_gate, w_up, w_down)


def shards(tokens_in, gain_attn, w_query, w_keyval, w_out, gain_mlp, w_gate, w_up, w_down):
    local_rows, width = tokens_in.shape
    total_rows = local_rows * lax.axis_size("dp")
    frequency = THETA ** (-np.arange(HD // 2) * 2.0 / HD)
    angles = np.arange(total_rows)[:, None] * frequency[None, :]
    cosine, sine = np.cos(angles), np.sin(angles)
    return layer(
        tokens_in,
        gain_attn.reshape(-1, 128),
        gain_mlp.reshape(-1, 128),
        jnp.asarray(np.concatenate([cosine, cosine], axis=1), F32),
        jnp.asarray(np.concatenate([-sine, sine], axis=1), F32),
        w_query,
        w_keyval,
        w_out,
        w_gate,
        w_up,
        w_down,
        1,
    )


def solution(mesh):
    placed = (
        P("dp", ("section", "tensor")),
        P(),
        P(None, ("section", "tensor")),
        P(None, ("section", "tensor")),
        P(("section", "tensor"), None),
        P(),
        P("dp", ("section", "tensor")),
        P("dp", ("section", "tensor")),
        P(("section", "tensor"), "dp"),
    )
    return jax.shard_map(
        shards,
        mesh=mesh,
        in_specs=placed,
        out_specs=P(("section", "tensor"), "dp"),
        check_vma=False,
    )
```
